128 devices in a mesh: dp: 1, hp: 16 (over z, y), cp: 8 (over x, core).
Axes of the slice: x: 4, y: 4, z: 4, core: 2. Of those that a mesh axis runs over, the one named last changes fastest.
Arguments:
- latent: bfloat16 [96, 16, 48, 512], P(('dp', 'cp'), 'hp')
- conv_w: bfloat16 [4, 3, 3, 3, 512, 512], replicated
- conv_b: float32 [4, 512], replicated
- gn_gamma: float32 [4, 512], replicated
- gn_beta: float32 [4, 512], replicated
Outputs:
- output: bfloat16 [96, 16, 48, 512], P(('dp', 'cp'), 'hp')
All inputs are finite; a program needn't handle non-finite values.
Results may differ from the reference program's by a relative error of at most 0.00972573.
Values are sent between devices in bfloat16 or wider.
A program may use at most 1 GiB of HBM per device.

```python
import jax
import jax.numpy as jnp
from jax import lax

FRAMES = 96
HEIGHT = 16
LAT_WIDTH = 48
CHANNELS = 512
GROUPS = 32
EPS = 1e-6


def setup_inputs(seed: int = 0, part: int = 0) -> dict:
    root_key = jax.random.key(seed)
    part_key = jax.random.fold_in(root_key, part)
    key_noise, key_fscale, key_fshift, key_rscale = jax.random.split(part_key, 4)
    key_kernel, key_bias, key_gamma, key_beta = jax.random.split(jax.random.key(seed + 1), 4)
    base_noise = jax.random.normal(key_noise, (FRAMES, HEIGHT, LAT_WIDTH, CHANNELS), jnp.float32)
    frame_scale = jnp.exp(0.5 * jax.random.normal(key_fscale, (FRAMES, 1, 1, 1), jnp.float32))
    frame_shift = 0.7 * jax.random.normal(key_fshift, (FRAMES, 1, 1, CHANNELS), jnp.float32)
    row_scale = jnp.exp(0.4 * jax.random.normal(key_rscale, (1, HEIGHT, 1, 1), jnp.float32))
    latent = ((base_noise + frame_shift) * frame_scale * row_scale).astype(jnp.bfloat16)
    fan_in = 27 * CHANNELS
    conv_w = (jax.random.normal(key_kernel, (4, 3, 3, 3, CHANNELS, CHANNELS), jnp.float32) * fan_in ** -0.5).astype(jnp.bfloat16)
    conv_b = 0.5 * jax.random.normal(key_bias, (4, CHANNELS), jnp.float32)
    gn_gamma = 1.0 + 0.3 * jax.random.normal(key_gamma, (4, CHANNELS), jnp.float32)
    gn_beta = 0.3 * jax.random.normal(key_beta, (4, CHANNELS), jnp.float32)
    return {"latent": latent, "conv_w": conv_w, "conv_b": conv_b, "gn_gamma": gn_gamma, "gn_beta": gn_beta}


def norm_silu(video, gamma, beta):
    per_group = CHANNELS // GROUPS
    grouped = video.reshape(FRAMES, HEIGHT, LAT_WIDTH, GROUPS, per_group).astype(jnp.float32)
    norm_count = FRAMES * HEIGHT * LAT_WIDTH * per_group
    mean_val = jnp.sum(grouped, axis=(0, 1, 2, 4)) / norm_count
    variance = jnp.sum(grouped * grouped, axis=(0, 1, 2, 4)) / norm_count - mean_val * mean_val
    inv_std = lax.rsqrt(variance + EPS)
    gamma_g = gamma.reshape(GROUPS, per_group)
    scale_c = (inv_std[:, None] * gamma_g).reshape(CHANNELS)
    shift_c = (beta.reshape(GROUPS, per_group) - (mean_val * inv_std)[:, None] * gamma_g).reshape(CHANNELS)
    return jax.nn.silu(video.astype(jnp.float32) * scale_c + shift_c).astype(jnp.bfloat16)


def causal_conv(video, kernel, bias_vec):
    padded = jnp.concatenate([video[:1], video[:1], video], axis=0)
    kernel_f = kernel.astype(jnp.float32)

    def one_frame(frame_idx):
        window = lax.dynamic_slice_in_dim(padded, frame_idx, 3, axis=0).astype(jnp.float32)
        conv_out = lax.conv_general_dilated(window[None], kernel_f, (1, 1, 1), ((0, 0), (1, 1), (1, 1)), dimension_numbers=("NDHWC", "DHWIO", "NDHWC"))
        return (conv_out[0, 0] + bias_vec).astype(jnp.bfloat16)

    return lax.map(one_frame, jnp.arange(FRAMES))


def reference(latent, conv_w, conv_b, gn_gamma, gn_beta):
    residual = latent
    for block_idx in range(2):
        hidden = residual
        for sub_idx in range(2):
            layer_idx = 2 * block_idx + sub_idx
            activated = norm_silu(hidden, gn_gamma[layer_idx], gn_beta[layer_idx])
            hidden = causal_conv(activated, conv_w[layer_idx], conv_b[layer_idx])
        residual = (residual.astype(jnp.float32) + hidden.astype(jnp.float32)).astype(jnp.bfloat16)
    return residual
```

```python
import functools

import jax
import jax.numpy as jnp
from jax import lax
from jax.experimental import pallas as pl
from jax.experimental.pallas import tpu as pltpu
from jax.sharding import PartitionSpec as P

GROUPS = 32
EPS = 1e-6
LAYERS = 4
MESH = pl.DeviceIdType.MESH
CHUNK = 3


def lane_sums(y, lane):
    for d in (8, 4, 2, 1):
        y = y + jnp.where((lane & d) != 0, pltpu.roll(y, d, 1), pltpu.roll(y, 128 - d, 1))
    return y


def decode_kernel(n_hp, n_cp, total_count, lat_ref, w_ref, b_ref, g_ref, be_ref, o_ref,
                  wbuf, raw, act, acc, xres, ssum, st8, coef, msg_a, msg_b, st_a, st_b,
                  w_sem, lat_sem, send_sem, recv_sem, ssend_a, srecv_a, ssend_b, srecv_b):
    frames, width, channels = xres.shape
    n_chunks = frames // CHUNK
    hp = lax.axis_index("hp")
    cp = lax.axis_index("cp")
    has_up = hp > 0
    has_down = hp < n_hp - 1
    has_next = cp < n_cp - 1
    has_prev = cp > 0

    slab_order = [(k, 1) for k in range(3)] + [(k, di) for di in (0, 2) for k in range(3)]

    def weight_copy(layer, slot, k, di):
        slab = k * 3 + di
        return pltpu.make_async_copy(w_ref.at[layer, slab], wbuf.at[slot, slab], w_sem.at[slot, slab])

    def start_weights(layer, slot):
        for k, di in slab_order:
            weight_copy(layer, slot, k, di).start()

    lat_copies = [pltpu.make_async_copy(lat_ref, raw.at[0, 1, pl.ds(2, frames)], lat_sem.at[0]),
                  pltpu.make_async_copy(lat_ref, xres, lat_sem.at[1])]
    for copy in lat_copies:
        copy.start()
    start_weights(0, 0)

    barrier = pltpu.get_barrier_semaphore()

    @pl.loop(1, n_cp)
    def _(i):
        pl.semaphore_signal(barrier, inc=1, device_id={"cp": lax.rem(cp + i, n_cp)}, device_id_type=MESH)

    @pl.loop(1, n_hp)
    def _(i):
        pl.semaphore_signal(barrier, inc=1, device_id={"hp": lax.rem(hp + i, n_hp)}, device_id_type=MESH)

    for dh, ok_h in ((-1, has_up), (1, has_down)):
        for dc, ok_c in ((-1, has_prev), (1, has_next)):
            @pl.when(jnp.logical_and(ok_h, ok_c))
            def _():
                pl.semaphore_signal(barrier, inc=1, device_id={"hp": hp + dh, "cp": cp + dc}, device_id_type=MESH)

    n_rows = has_up.astype(jnp.int32) + has_down.astype(jnp.int32)
    n_times = has_prev.astype(jnp.int32) + has_next.astype(jnp.int32)
    pl.semaphore_wait(barrier, n_cp - 1 + n_hp - 1 + n_rows * n_times)

    def row_copy(slot, c, to_down):
        span = pl.ds(2 + c * CHUNK, CHUNK)
        row = 0 if to_down else 2
        return pltpu.make_async_remote_copy(
            src_ref=raw.at[slot, 1, span], dst_ref=raw.at[slot, row, span],
            send_sem=send_sem.at[row, c], recv_sem=recv_sem.at[slot, row, c],
            device_id={"hp": hp + (1 if to_down else -1)}, device_id_type=MESH)

    def time_copy(slot, dh):
        row = dh if dh is None else (0 if dh == 1 else 2)
        row = 1 if dh == 0 else row
        return pltpu.make_async_remote_copy(
            src_ref=raw.at[slot, 1, pl.ds(frames, 2)], dst_ref=raw.at[slot, row, pl.ds(0, 2)],
            send_sem=send_sem.at[row, n_chunks], recv_sem=recv_sem.at[slot, row, n_chunks],
            device_id={"hp": hp + dh, "cp": cp + 1}, device_id_type=MESH)

    def start_rows(slot, c):
        @pl.when(has_up)
        def _():
            row_copy(slot, c, False).start()

        @pl.when(has_down)
        def _():
            row_copy(slot, c, True).start()

    def start_times(slot):
        @pl.when(has_next)
        def _():
            time_copy(slot, 0).start()

        @pl.when(jnp.logical_and(has_next, has_up))
        def _():
            time_copy(slot, -1).start()

        @pl.when(jnp.logical_and(has_next, has_down))
        def _():
            time_copy(slot, 1).start()

    def wait_sends(slot):
        for c in range(n_chunks):
            @pl.when(has_up)
            def _():
                row_copy(slot, c, False).wait_send()

            @pl.when(has_down)
            def _():
                row_copy(slot, c, True).wait_send()

        @pl.when(has_next)
        def _():
            time_copy(slot, 0).wait_send()

        @pl.when(jnp.logical_and(has_next, has_up))
        def _():
            time_copy(slot, -1).wait_send()

        @pl.when(jnp.logical_and(has_next, has_down))
        def _():
            time_copy(slot, 1).wait_send()

    for copy in lat_copies:
        copy.wait()
    start_times(0)
    for c in range(n_chunks):
        start_rows(0, c)

    for row, ok in ((0, has_up), (2, has_down)):
        @pl.when(jnp.logical_not(ok))
        def _():
            @pl.loop(0, frames + 2)
            def _(f):
                act[row, f] = jnp.zeros((width, 3 * channels), jnp.bfloat16)

    def fold(v):
        return jnp.sum(v.reshape(-1, 8, v.shape[-1]), axis=0)

    ssum[...] = jnp.zeros_like(ssum)

    @pl.loop(0, frames)
    def _(f):
        v = xres[f].astype(jnp.float32)
        ssum[0] += fold(v)
        ssum[1] += fold(v * v)

    lane = lax.broadcasted_iota(jnp.int32, (8, 128), 1)
    sub = lax.broadcasted_iota(jnp.int32, (8, 128), 0)
    pick = (lane & 15) == sub

    def exchange(layer, axis, n, me, msg, st, send, recv):
        @pl.loop(1, n)
        def _(i):
            pltpu.make_async_remote_copy(
                src_ref=msg.at[layer], dst_ref=st.at[layer, me], send_sem=send.at[layer], recv_sem=recv.at[layer],
                device_id={axis: lax.rem(me + i, n)}, device_id_type=MESH).start()

        st[layer, me] = msg[layer]
        rest = st.at[layer, pl.ds(0, n - 1)]
        pltpu.make_async_copy(rest, rest, recv.at[layer]).wait()
        pltpu.make_async_copy(rest, rest, send.at[layer]).wait()
        return jnp.sum(st[layer], axis=0)

    def statistics(layer):
        for s in range(2):
            for i in range(4):
                st8[s * 4 + i : s * 4 + i + 1, :] = jnp.sum(ssum[s, :, i * 128 : (i + 1) * 128], axis=0, keepdims=True)
        mine = jnp.where(pick, lane_sums(st8[...], lane), 0.0)
        msg_a[layer] = jnp.sum(mine, axis=0, keepdims=True)
        msg_b[layer] = exchange(layer, "cp", n_cp, cp, msg_a, st_a, ssend_a, srecv_a)
        total = exchange(layer, "hp", n_hp, hp, msg_b, st_b, ssend_b, srecv_b)
        st8[...] = lane_sums(jnp.where(pick, jnp.broadcast_to(total, (8, 128)), 0.0), lane)
        mean = st8[0:4, :] / total_count
        var = st8[4:8, :] / total_count - mean * mean
        inv = lax.rsqrt(var + EPS)
        scale = g_ref[layer] * inv
        shift = be_ref[layer] - (mean * inv) * g_ref[layer]
        for i in range(4):
            coef[0:1, i * 128 : (i + 1) * 128] = 0.5 * scale[i : i + 1, :]
            coef[1:2, i * 128 : (i + 1) * 128] = 0.5 * shift[i : i + 1, :]

    first_frame = jnp.where(has_prev, 0, 2)
    col = lax.broadcasted_iota(jnp.int32, (width, channels), 0)

    def activate(slot, row, f):
        v = raw[slot, row, jnp.maximum(f, first_frame)].astype(jnp.float32)
        u = v * coef[0:1, :] + coef[1:2, :]
        y = u * jnp.tanh(u) + u
        left = jnp.where(col == 0, 0.0, pltpu.roll(y, 1, 0))
        right = jnp.where(col == width - 1, 0.0, pltpu.roll(y, width - 1, 0))
        for dj, v in enumerate((left, y, right)):
            act[row, f, :, dj * channels : (dj + 1) * channels] = v.astype(jnp.bfloat16)

    def taps(slot, di, start, count):
        total = None
        for d in di:
            for k in range(3):
                lhs = act[d, pl.ds(start + k, count)].reshape(count * width, 3 * channels)
                part = jnp.dot(lhs, wbuf[slot, k * 3 + d], preferred_element_type=jnp.float32)
                total = part if total is None else total + part
        return total

    def layer_body(layer, _):
        slot = lax.rem(layer, 2)
        other = 1 - slot

        @pl.when(layer < LAYERS - 1)
        def _():
            start_weights(layer + 1, other)

        statistics(layer)

        @pl.when(has_prev)
        def _():
            time_copy(slot, 0).wait_recv()

        @pl.loop(0, frames + 2)
        def _(f):
            activate(slot, 1, f)

        for k, di in slab_order:
            weight_copy(layer, slot, k, di).wait()

        half = frames // 2

        @pl.loop(0, 2)
        def _(h):
            acc[pl.ds(h * half, half)] = taps(slot, (1,), h * half, half).reshape(half, width, channels)

        for row, ok in ((0, has_up), (2, has_down)):
            @pl.when(ok)
            def _():
                @pl.when(has_prev)
                def _():
                    time_copy(slot, 1 if row == 0 else -1).wait_recv()

                for c in range(n_chunks):
                    row_copy(slot, c, row == 0).wait_recv()

                @pl.loop(0, frames + 2)
                def _(f):
                    activate(slot, row, f)

        wait_sends(slot)
        ssum[...] = jnp.zeros_like(ssum)
        second = lax.rem(layer, 2) == 1
        bias = b_ref[layer]
        @pl.loop(0, n_chunks)
        def _(c):
            span = pl.ds(c * CHUNK, CHUNK)
            y = taps(slot, (0, 2), c * CHUNK, CHUNK).reshape(CHUNK, width, channels)
            h = (acc[span] + y + bias).astype(jnp.bfloat16).astype(jnp.float32)
            x = xres[span].astype(jnp.float32)
            out = (h + jnp.where(second, x, 0.0)).astype(jnp.bfloat16)
            raw[other, 1, pl.ds(2 + c * CHUNK, CHUNK)] = out
            out = out.astype(jnp.float32)
            xres[span] = jnp.where(second, out, x).astype(jnp.bfloat16)
            ssum[0] += fold(out)
            ssum[1] += fold(out * out)

            @pl.when(layer < LAYERS - 1)
            def _():
                start_rows(other, c)

        @pl.when(layer < LAYERS - 1)
        def _():
            start_times(other)

        return 0

    lax.fori_loop(0, LAYERS, layer_body, 0)

    @pl.loop(0, frames)
    def _(f):
        o_ref[f] = xres[f]


def solution(mesh):
    n_hp, n_cp = mesh.shape["hp"], mesh.shape["cp"]

    def local_decode(lat, conv_w, conv_b, gn_gamma, gn_beta):
        frames, rows, width, channels = lat.shape
        n_chunks = frames // CHUNK
        total_count = float(frames * n_cp * rows * n_hp * width * (channels // GROUPS))
        any_spec = pl.BlockSpec(memory_space=pl.ANY)
        vmem_spec = pl.BlockSpec(memory_space=pltpu.VMEM)
        bf16, f32 = jnp.bfloat16, jnp.float32
        flops = LAYERS * 2 * frames * width * 27 * channels * channels
        out = pl.pallas_call(
            functools.partial(decode_kernel, n_hp, n_cp, total_count),
            out_shape=jax.ShapeDtypeStruct((frames, width, channels), bf16),
            in_specs=[any_spec, any_spec, vmem_spec, vmem_spec, vmem_spec],
            out_specs=vmem_spec,
            scratch_shapes=[
                pltpu.VMEM((2, 9, 3 * channels, channels), bf16),
                pltpu.VMEM((2, 3, frames + 2, width, channels), bf16),
                pltpu.VMEM((3, frames + 2, width, 3 * channels), bf16),
                pltpu.VMEM((frames, width, channels), f32),
                pltpu.VMEM((frames, width, channels), bf16),
                pltpu.VMEM((2, 8, channels), f32),
                pltpu.VMEM((8, 128), f32),
                pltpu.VMEM((8, channels), f32),
                pltpu.VMEM((LAYERS, 1, 128), f32),
                pltpu.VMEM((LAYERS, 1, 128), f32),
                pltpu.VMEM((LAYERS, n_cp, 1, 128), f32),
                pltpu.VMEM((LAYERS, n_hp, 1, 128), f32),
                pltpu.SemaphoreType.DMA((2, 9)),
                pltpu.SemaphoreType.DMA((2,)),
                pltpu.SemaphoreType.DMA((3, n_chunks + 1)),
                pltpu.SemaphoreType.DMA((2, 3, n_chunks + 1)),
                pltpu.SemaphoreType.DMA((LAYERS,)),
                pltpu.SemaphoreType.DMA((LAYERS,)),
                pltpu.SemaphoreType.DMA((LAYERS,)),
                pltpu.SemaphoreType.DMA((LAYERS,)),
            ],
            compiler_params=pltpu.CompilerParams(
                collective_id=0, has_side_effects=True, vmem_limit_bytes=60 * 1024 * 1024),
            cost_estimate=pl.CostEstimate(flops=flops, bytes_accessed=conv_w.size * 2, transcendentals=0),
        )(lat.reshape(frames, width, channels), conv_w.reshape(LAYERS, 9, 3 * channels, channels),
          conv_b.reshape(LAYERS, 1, channels), gn_gamma.reshape(LAYERS, channels // 128, 128),
          gn_beta.reshape(LAYERS, channels // 128, 128))
        return out.reshape(lat.shape)

    video_spec = P(("dp", "cp"), "hp", None, None)
    return jax.shard_map(local_decode, mesh=mesh, in_specs=(video_spec, P(), P(), P(), P()), out_specs=video_spec, check_vma=False)
```

```python
import functools

import jax
import jax.numpy as jnp
from jax import lax
from jax.experimental import pallas as pl
from jax.experimental.pallas import tpu as pltpu
from jax.sharding import PartitionSpec as P

GROUPS = 32
EPS = 1e-6
LAYERS = 4
MESH = pl.DeviceIdType.MESH
CHUNK = 3


def lane_sums(y, lane):
    for d in (8, 4, 2, 1):
        y = y + jnp.where((lane & d) != 0, pltpu.roll(y, d, 1), pltpu.roll(y, 128 - d, 1))
    return y


def decode_kernel(n_hp, n_cp, total_count, lat_ref, w_ref, b_ref, g_ref, be_ref, o_ref,
                  wbuf, raw, act, acc, xres, params, ssum, st8, coef, msg, peers,
                  w_sem, lat_sem, send_sem, recv_sem, msg_send, msg_recv):
    frames, width, channels = xres.shape
    n_chunks = frames // CHUNK
    hp = lax.axis_index("hp")
    cp = lax.axis_index("cp")
    has_up = hp > 0
    has_down = hp < n_hp - 1
    has_next = cp < n_cp - 1
    has_prev = cp > 0

    for i, ref in enumerate((b_ref, g_ref, be_ref)):
        for layer in range(LAYERS):
            params[i, layer] = ref[layer : layer + 1, :]

    slab_order = [(k, 1) for k in range(3)] + [(k, di) for di in (0, 2) for k in range(3)]

    def weight_copy(layer, slot, k, di):
        slab = k * 3 + di
        return pltpu.make_async_copy(w_ref.at[layer, slab], wbuf.at[slot, slab], w_sem.at[slot, slab])

    def start_weights(layer, slot):
        for k, di in slab_order:
            weight_copy(layer, slot, k, di).start()

    lat_copies = [pltpu.make_async_copy(lat_ref, raw.at[0, 1, pl.ds(2, frames)], lat_sem.at[0]),
                  pltpu.make_async_copy(lat_ref, xres, lat_sem.at[1])]
    for copy in lat_copies:
        copy.start()
    start_weights(0, 0)

    def others(visit):
        @pl.loop(0, n_hp)
        def _(i):
            for j in range(n_cp):
                target = {"hp": lax.rem(hp + n_hp // 2 + i, n_hp), "cp": lax.rem(cp + n_cp // 2 + j, n_cp)}
                if j == n_cp // 2:
                    pl.when(i != n_hp // 2)(functools.partial(visit, target))
                else:
                    visit(target)

    barrier = pltpu.get_barrier_semaphore()
    with jax.named_scope("entry_signals"):
        others(lambda target: pl.semaphore_signal(barrier, inc=1, device_id=target, device_id_type=MESH))

    def row_copy(slot, c, to_down):
        span = pl.ds(2 + c * CHUNK, CHUNK)
        row = 0 if to_down else 2
        return pltpu.make_async_remote_copy(
            src_ref=raw.at[slot, 1, span], dst_ref=raw.at[slot, row, span],
            send_sem=send_sem.at[row, c], recv_sem=recv_sem.at[slot, row, c],
            device_id={"hp": hp + (1 if to_down else -1)}, device_id_type=MESH)

    def time_copy(slot, dh):
        row = dh if dh is None else (0 if dh == 1 else 2)
        row = 1 if dh == 0 else row
        return pltpu.make_async_remote_copy(
            src_ref=raw.at[slot, 1, pl.ds(frames, 2)], dst_ref=raw.at[slot, row, pl.ds(0, 2)],
            send_sem=send_sem.at[row, n_chunks], recv_sem=recv_sem.at[slot, row, n_chunks],
            device_id={"hp": hp + dh, "cp": cp + 1}, device_id_type=MESH)

    def start_rows(slot, c):
        @pl.when(has_up)
        def _():
            row_copy(slot, c, False).start()

        @pl.when(has_down)
        def _():
            row_copy(slot, c, True).start()

    def start_times(slot):
        @pl.when(has_next)
        def _():
            time_copy(slot, 0).start()

        @pl.when(jnp.logical_and(has_next, has_up))
        def _():
            time_copy(slot, -1).start()

        @pl.when(jnp.logical_and(has_next, has_down))
        def _():
            time_copy(slot, 1).start()

    def wait_sends(slot):
        for c in range(n_chunks):
            @pl.when(has_up)
            def _():
                row_copy(slot, c, False).wait_send()

            @pl.when(has_down)
            def _():
                row_copy(slot, c, True).wait_send()

        @pl.when(has_next)
        def _():
            time_copy(slot, 0).wait_send()

        @pl.when(jnp.logical_and(has_next, has_up))
        def _():
            time_copy(slot, -1).wait_send()

        @pl.when(jnp.logical_and(has_next, has_down))
        def _():
            time_copy(slot, 1).wait_send()

    for row, ok in ((0, has_up), (2, has_down)):
        @pl.when(jnp.logical_not(ok))
        def _():
            @pl.loop(0, frames + 2)
            def _(f):
                for slot in range(2):
                    raw[slot, row, f] = jnp.zeros((width, channels), jnp.bfloat16)

    @pl.when(jnp.logical_not(has_prev))
    def _():
        for slot in range(2):
            for row in range(3):
                for f in range(2):
                    raw[slot, row, f] = jnp.zeros((width, channels), jnp.bfloat16)

    with jax.named_scope("lat_wait"):
        for copy in lat_copies:
            copy.wait()

    def fold(v):
        return jnp.sum(v.reshape(-1, 8, v.shape[-1]), axis=0)

    ssum[...] = jnp.zeros_like(ssum)

    @pl.loop(0, frames)
    def _(f):
        v = xres[f].astype(jnp.float32)
        ssum[0] += fold(v)
        ssum[1] += fold(v * v)

    lane = lax.broadcasted_iota(jnp.int32, (8, 128), 1)
    sub = lax.broadcasted_iota(jnp.int32, (8, 128), 0)
    pick = (lane & 15) == sub

    me = hp * n_cp + cp

    def send_sums(layer):
        for s in range(2):
            for i in range(4):
                st8[s * 4 + i : s * 4 + i + 1, :] = jnp.sum(ssum[s, :, i * 128 : (i + 1) * 128], axis=0, keepdims=True)
        mine = jnp.where(pick, lane_sums(st8[...], lane), 0.0)
        msg[layer] = jnp.sum(mine, axis=0, keepdims=True)
        peers[layer, me] = msg[layer]
        others(lambda target: pltpu.make_async_remote_copy(
            src_ref=msg.at[layer], dst_ref=peers.at[layer, me], send_sem=msg_send.at[layer], recv_sem=msg_recv.at[layer],
            device_id=target, device_id_type=MESH).start())

    def statistics(layer):
        rest = peers.at[layer, pl.ds(0, n_hp * n_cp - 1)]
        pltpu.make_async_copy(rest, rest, msg_recv.at[layer]).wait()
        pltpu.make_async_copy(rest, rest, msg_send.at[layer]).wait()
        total = jnp.sum(peers[layer], axis=0)
        st8[...] = lane_sums(jnp.where(pick, jnp.broadcast_to(total, (8, 128)), 0.0), lane)
        mean = st8[0:4, :] / total_count
        var = st8[4:8, :] / total_count - mean * mean
        inv = lax.rsqrt(var + EPS)
        st8[0:4, :] = inv
        st8[4:8, :] = mean * inv
        for i in range(4):
            lanes = slice(i * 128, (i + 1) * 128)
            gamma = 0.5 * params[1, layer, :, lanes]
            scale = gamma * st8[i : i + 1, :]
            shift = 0.5 * params[2, layer, :, lanes] - st8[4 + i : 5 + i, :] * gamma
            for row, ok in ((0, has_up), (1, None), (2, has_down)):
                coef[row, 0:1, lanes] = scale if ok is None else jnp.where(ok, scale, 0.0)
                coef[row, 1:2, lanes] = shift if ok is None else jnp.where(ok, shift, 0.0)

    first_frame = jnp.where(has_prev, 0, 2)
    col = lax.broadcasted_iota(jnp.int32, (width, channels), 0)

    def activate(slot, row, f):
        v = raw[slot, row, jnp.maximum(f, first_frame)].astype(jnp.float32)
        u = v * coef[row, 0:1, :] + coef[row, 1:2, :]
        y = u * jnp.tanh(u) + u
        left = jnp.where(col == 0, 0.0, pltpu.roll(y, 1, 0))
        right = jnp.where(col == width - 1, 0.0, pltpu.roll(y, width - 1, 0))
        for dj, v in enumerate((left, y, right)):
            act[row, f, :, dj * channels : (dj + 1) * channels] = v.astype(jnp.bfloat16)

    def taps(slot, di, start, count):
        total = None
        for d in di:
            for k in range(3):
                lhs = act[d, pl.ds(start + k, count)].reshape(count * width, 3 * channels)
                part = jnp.dot(lhs, wbuf[slot, k * 3 + d], preferred_element_type=jnp.float32)
                total = part if total is None else total + part
        return total

    def halo_wait(slot, c):
        for row, ok in ((0, has_up), (2, has_down)):
            if c == 0:
                @pl.when(jnp.logical_and(ok, has_prev))
                def _():
                    time_copy(slot, 1 if row == 0 else -1).wait_recv()

            @pl.when(ok)
            def _():
                row_copy(slot, c, row == 0).wait_recv()

    def halo_act(slot, c):
        for f in range(2 + c * CHUNK if c else 0, 2 + (c + 1) * CHUNK):
            for row in (0, 2):
                activate(slot, row, f)

    def finish(layer, other, c):
        second = lax.rem(layer, 2) == 1
        for f in range(c * CHUNK, (c + 1) * CHUNK):
            h = (acc[f] + params[0, layer]).astype(jnp.bfloat16).astype(jnp.float32)
            x = xres[f].astype(jnp.float32)
            out = (h + jnp.where(second, x, 0.0)).astype(jnp.bfloat16)
            raw[other, 1, 2 + f] = out
            out = out.astype(jnp.float32)
            xres[f] = jnp.where(second, out, x).astype(jnp.bfloat16)
            ssum[0] += fold(out)
            ssum[1] += fold(out * out)

    with jax.named_scope("entry_wait"):
        pl.semaphore_wait(barrier, n_hp * n_cp - 1)
    with jax.named_scope("send_sums"):
        send_sums(0)
    start_times(0)
    for c in range(n_chunks):
        start_rows(0, c)

    def layer_body(layer, _):
        slot = lax.rem(layer, 2)
        other = 1 - slot
        more = layer < LAYERS - 1

        @pl.when(more)
        def _():
            start_weights(layer + 1, other)

        with jax.named_scope("statistics"):
            statistics(layer)

        with jax.named_scope("act_own"):
            @pl.when(has_prev)
            def _():
                time_copy(slot, 0).wait_recv()

            @pl.loop(0, frames + 2)
            def _(f):
                activate(slot, 1, f)

        with jax.named_scope("w_wait"):
            for k, di in slab_order:
                weight_copy(layer, slot, k, di).wait()

        half = frames // 2
        with jax.named_scope("own0"):
            acc[0:half] = taps(slot, (1,), 0, half).reshape(half, width, channels)
        with jax.named_scope("halo_wait0"):
            halo_wait(slot, 0)
        with jax.named_scope("own1"):
            halo_act(slot, 0)
            acc[half:frames] = taps(slot, (1,), half, half).reshape(half, width, channels)
        with jax.named_scope("send_wait"):
            wait_sends(slot)
        ssum[...] = jnp.zeros_like(ssum)
        for c in range(n_chunks):
            if c < n_chunks - 1:
                with jax.named_scope(f"halo_wait{c + 1}"):
                    halo_wait(slot, c + 1)
            span = slice(c * CHUNK, (c + 1) * CHUNK)
            with jax.named_scope(f"chunk{c}"):
                if c > 0:
                    finish(layer, other, c - 1)
                if c < n_chunks - 1:
                    halo_act(slot, c + 1)
                acc[span] += taps(slot, (0, 2), c * CHUNK, CHUNK).reshape(CHUNK, width, channels)
            if c == 1:
                @pl.when(more)
                def _():
                    start_rows(other, 0)

        with jax.named_scope("finish"):
            finish(layer, other, n_chunks - 1)

        @pl.when(more)
        def _():
            with jax.named_scope("send_sums"):
                send_sums(layer + 1)
            with jax.named_scope("send_rest"):
                start_times(other)
                for c in range(1, n_chunks):
                    start_rows(other, c)

        return 0

    lax.fori_loop(0, LAYERS, layer_body, 0)

    @pl.loop(0, frames)
    def _(f):
        o_ref[f] = xres[f]


def solution(mesh):
    n_hp, n_cp = mesh.shape["hp"], mesh.shape["cp"]

    def local_decode(lat, conv_w, conv_b, gn_gamma, gn_beta):
        frames, rows, width, channels = lat.shape
        n_chunks = frames // CHUNK
        total_count = float(frames * n_cp * rows * n_hp * width * (channels // GROUPS))
        any_spec = pl.BlockSpec(memory_space=pl.ANY)
        vmem_spec = pl.BlockSpec(memory_space=pltpu.VMEM)
        bf16, f32 = jnp.bfloat16, jnp.float32
        flops = LAYERS * 2 * frames * width * 27 * channels * channels
        out = pl.pallas_call(
            functools.partial(decode_kernel, n_hp, n_cp, total_count),
            out_shape=jax.ShapeDtypeStruct((frames, width, channels), bf16),
            in_specs=[any_spec, any_spec, vmem_spec, vmem_spec, vmem_spec],
            out_specs=vmem_spec,
            scratch_shapes=[
                pltpu.VMEM((2, 9, 3 * channels, channels), bf16),
                pltpu.VMEM((2, 3, frames + 2, width, channels), bf16),
                pltpu.VMEM((3, frames + 2, width, 3 * channels), bf16),
                pltpu.VMEM((frames, width, channels), f32),
                pltpu.VMEM((frames, width, channels), bf16),
                pltpu.VMEM((3, LAYERS, 1, channels), f32),
                pltpu.VMEM((2, 8, channels), f32),
                pltpu.VMEM((8, 128), f32),
                pltpu.VMEM((3, 8, channels), f32),
                pltpu.VMEM((LAYERS, 1, 128), f32),
                pltpu.VMEM((LAYERS, n_hp * n_cp, 1, 128), f32),
                pltpu.SemaphoreType.DMA((2, 9)),
                pltpu.SemaphoreType.DMA((2,)),
                pltpu.SemaphoreType.DMA((3, n_chunks + 1)),
                pltpu.SemaphoreType.DMA((2, 3, n_chunks + 1)),
                pltpu.SemaphoreType.DMA((LAYERS,)),
                pltpu.SemaphoreType.DMA((LAYERS,)),
            ],
            compiler_params=pltpu.CompilerParams(
                collective_id=0, has_side_effects=True, vmem_limit_bytes=60 * 1024 * 1024),
            cost_estimate=pl.CostEstimate(flops=flops, bytes_accessed=conv_w.size * 2, transcendentals=0),
        )(lat.reshape(frames, width, channels), conv_w.reshape(LAYERS, 9, 3 * channels, channels),
          conv_b, gn_gamma, gn_beta)
        return out.reshape(lat.shape)

    video_spec = P(("dp", "cp"), "hp", None, None)
    return jax.shard_map(local_decode, mesh=mesh, in_specs=(video_spec, P(), P(), P(), P()), out_specs=video_spec, check_vma=False)
```

```python
import functools

import jax
import jax.numpy as jnp
from jax import lax
from jax.experimental import pallas as pl
from jax.experimental.pallas import tpu as pltpu
from jax.sharding import PartitionSpec as P

GROUPS = 32
EPS = 1e-6
LAYERS = 4
MESH = pl.DeviceIdType.MESH
CHUNK = 3
OWN = 4


def lane_sums(y, lane):
    for s in (1, 4):
        place = (lane // s) & 3
        total = y
        for d in (-3, -2, -1, 1, 2, 3):
            inside = jnp.logical_and(place + d >= 0, place + d <= 3)
            total = total + jnp.where(inside, pltpu.roll(y, (-d * s) % 128, 1), 0.0)
        y = total
    return y


def tree_sum(terms):
    while len(terms) > 1:
        terms = [a + b for a, b in zip(terms[::2], terms[1::2])] + terms[len(terms) & ~1 :]
    return terms[0]


def decode_kernel(n_hp, n_cp, total_count, lat_ref, w_ref, b_ref, g_ref, be_ref, o_ref,
                  wbuf, raw, act, acc, xres, small, params, ssum, st8, coef, msg, peers,
                  w_sem, lat_sem, small_sem, send_sem, recv_sem, msg_send, msg_recv):
    frames, width, channels = xres.shape
    n_chunks = frames // CHUNK
    hp = lax.axis_index("hp")
    cp = lax.axis_index("cp")
    has_up = hp > 0
    has_down = hp < n_hp - 1
    has_next = cp < n_cp - 1
    has_prev = cp > 0

    slab_order = [(k, 1) for k in range(3)] + [(k, di) for di in (0, 2) for k in range(3)]

    def weight_copy(layer, slot, k, di):
        slab = k * 3 + di
        return pltpu.make_async_copy(w_ref.at[layer, slab], wbuf.at[slot, slab], w_sem.at[slot, slab])

    def start_weights(layer, slot):
        for k, di in slab_order:
            weight_copy(layer, slot, k, di).start()

    lat_copies = [pltpu.make_async_copy(lat_ref, raw.at[0, 1, pl.ds(2, frames)], lat_sem.at[0]),
                  pltpu.make_async_copy(lat_ref, xres, lat_sem.at[1])]
    small_copies = [pltpu.make_async_copy(ref, small.at[i], small_sem.at[i]) for i, ref in enumerate((b_ref, g_ref, be_ref))]
    for copy in lat_copies + small_copies:
        copy.start()

    def others(visit):
        @pl.loop(0, n_hp)
        def _(i):
            for j in range(n_cp):
                target = {"hp": lax.rem(hp + n_hp // 2 + i, n_hp), "cp": lax.rem(cp + n_cp // 2 + j, n_cp)}
                if j == n_cp // 2:
                    pl.when(i != n_hp // 2)(functools.partial(visit, target))
                else:
                    visit(target)

    barrier = pltpu.get_barrier_semaphore()
    with jax.named_scope("entry_signals"):
        others(lambda target: pl.semaphore_signal(barrier, inc=1, device_id=target, device_id_type=MESH))

    def row_copy(slot, c, to_down):
        span = pl.ds(2 + c * CHUNK, CHUNK)
        row = 0 if to_down else 2
        return pltpu.make_async_remote_copy(
            src_ref=raw.at[slot, 1, span], dst_ref=raw.at[slot, row, span],
            send_sem=send_sem.at[slot, row, c], recv_sem=recv_sem.at[slot, row, c],
            device_id={"hp": hp + (1 if to_down else -1)}, device_id_type=MESH)

    def time_copy(slot, dh):
        row = dh if dh is None else (0 if dh == 1 else 2)
        row = 1 if dh == 0 else row
        return pltpu.make_async_remote_copy(
            src_ref=raw.at[slot, 1, pl.ds(frames, 2)], dst_ref=raw.at[slot, row, pl.ds(0, 2)],
            send_sem=send_sem.at[slot, row, n_chunks], recv_sem=recv_sem.at[slot, row, n_chunks],
            device_id={"hp": hp + dh, "cp": cp + 1}, device_id_type=MESH)

    def start_rows(slot, c):
        @pl.when(has_up)
        def _():
            row_copy(slot, c, False).start()

        @pl.when(has_down)
        def _():
            row_copy(slot, c, True).start()

    def start_times(slot):
        @pl.when(has_next)
        def _():
            time_copy(slot, 0).start()

        @pl.when(jnp.logical_and(has_next, has_up))
        def _():
            time_copy(slot, -1).start()

        @pl.when(jnp.logical_and(has_next, has_down))
        def _():
            time_copy(slot, 1).start()

    def wait_sends(slot):
        for c in range(n_chunks):
            @pl.when(has_up)
            def _():
                row_copy(slot, c, False).wait_send()

            @pl.when(has_down)
            def _():
                row_copy(slot, c, True).wait_send()

        @pl.when(has_next)
        def _():
            time_copy(slot, 0).wait_send()

        @pl.when(jnp.logical_and(has_next, has_up))
        def _():
            time_copy(slot, -1).wait_send()

        @pl.when(jnp.logical_and(has_next, has_down))
        def _():
            time_copy(slot, 1).wait_send()

    for row, ok in ((0, has_up), (2, has_down)):
        @pl.when(jnp.logical_not(ok))
        def _():
            @pl.loop(0, frames + 2)
            def _(f):
                for slot in range(2):
                    raw[slot, row, f] = jnp.zeros((width, channels), jnp.bfloat16)

    @pl.when(jnp.logical_not(has_prev))
    def _():
        for slot in range(2):
            for row in range(3):
                for f in range(2):
                    raw[slot, row, f] = jnp.zeros((width, channels), jnp.bfloat16)

    with jax.named_scope("lat_wait"):
        for copy in lat_copies:
            copy.wait()
    start_weights(0, 0)

    def fold(v):
        return jnp.sum(v.reshape(-1, 8, v.shape[-1]), axis=0)

    ssum[...] = jnp.zeros_like(ssum)

    @pl.loop(0, frames)
    def _(f):
        v = xres[f].astype(jnp.float32)
        ssum[0] += fold(v)
        ssum[1] += fold(v * v)

    lane = lax.broadcasted_iota(jnp.int32, (8, 128), 1)
    sub = lax.broadcasted_iota(jnp.int32, (8, 128), 0)
    pick = (lane & 15) == sub

    me = hp * n_cp + cp

    def send_sums(layer):
        for s in range(2):
            for i in range(4):
                st8[s * 4 + i : s * 4 + i + 1, :] = jnp.sum(ssum[s, :, i * 128 : (i + 1) * 128], axis=0, keepdims=True)
        mine = jnp.where(pick, lane_sums(st8[...], lane), 0.0)
        msg[layer] = jnp.sum(mine, axis=0, keepdims=True)
        peers[layer, me] = msg[layer]
        others(lambda target: pltpu.make_async_remote_copy(
            src_ref=msg.at[layer], dst_ref=peers.at[layer, me], send_sem=msg_send.at[layer], recv_sem=msg_recv.at[layer],
            device_id=target, device_id_type=MESH).start())

    def statistics(layer):
        rest = peers.at[layer, pl.ds(0, n_hp * n_cp - 1)]
        pltpu.make_async_copy(rest, rest, msg_recv.at[layer]).wait()
        pltpu.make_async_copy(rest, rest, msg_send.at[layer]).wait()
        total = tree_sum([peers[layer, i] for i in range(n_hp * n_cp)])
        st8[...] = lane_sums(jnp.where(pick, jnp.broadcast_to(total, (8, 128)), 0.0), lane)
        mean = st8[0:4, :] * (1.0 / total_count)
        var = st8[4:8, :] * (1.0 / total_count) - mean * mean
        inv = lax.rsqrt(var + EPS)
        st8[0:4, :] = inv
        st8[4:8, :] = mean * inv
        for i in range(4):
            lanes = slice(i * 128, (i + 1) * 128)
            gamma = 0.5 * params[1, layer, :, lanes]
            scale = gamma * st8[i : i + 1, :]
            shift = 0.5 * params[2, layer, :, lanes] - st8[4 + i : 5 + i, :] * gamma
            for row, ok in ((0, has_up), (1, None), (2, has_down)):
                coef[row, 0:1, lanes] = scale if ok is None else jnp.where(ok, scale, 0.0)
                coef[row, 1:2, lanes] = shift if ok is None else jnp.where(ok, shift, 0.0)

    first_frame = jnp.where(has_prev, 0, 2)
    col = lax.broadcasted_iota(jnp.int32, (width, channels), 0)

    def activate(slot, row, f):
        v = raw[slot, row, jnp.maximum(f, first_frame)].astype(jnp.float32)
        u = v * coef[row, 0:1, :] + coef[row, 1:2, :]
        y = u * jnp.tanh(u) + u
        left = jnp.where(col == 0, 0.0, pltpu.roll(y, 1, 0))
        right = jnp.where(col == width - 1, 0.0, pltpu.roll(y, width - 1, 0))
        for dj, v in enumerate((left, y, right)):
            act[row, f, :, dj * channels : (dj + 1) * channels] = v.astype(jnp.bfloat16)

    def taps(slot, di, start, count, side=()):
        side = list(side)
        parts = [(d, k) for d in di for k in range(3)]
        total = None
        for n, (d, k) in enumerate(parts):
            lhs = act[d, start + k : start + k + count].reshape(count * width, 3 * channels)
            part = jnp.dot(lhs, wbuf[slot, k * 3 + d], preferred_element_type=jnp.float32)
            total = part if total is None else total + part
            for work in side[len(side) * n // len(parts) : len(side) * (n + 1) // len(parts)]:
                work()
        return total.reshape(count, width, channels)

    def halo_wait(slot, c):
        for row, ok in ((0, has_up), (2, has_down)):
            if c == 0:
                @pl.when(jnp.logical_and(ok, has_prev))
                def _():
                    time_copy(slot, 1 if row == 0 else -1).wait_recv()

            @pl.when(ok)
            def _():
                row_copy(slot, c, row == 0).wait_recv()

    def halo_act(slot, c):
        frames_in = range(2 + c * CHUNK if c else 0, 2 + (c + 1) * CHUNK)
        return [functools.partial(activate, slot, row, f) for f in frames_in for row in (0, 2)]

    def finish(layer, other, c):
        second = lax.rem(layer, 2) == 1

        def one(f):
            h = (acc[f] + params[0, layer]).astype(jnp.bfloat16).astype(jnp.float32)
            x = xres[f].astype(jnp.float32)
            out = (h + jnp.where(second, x, 0.0)).astype(jnp.bfloat16)
            raw[other, 1, 2 + f] = out
            out = out.astype(jnp.float32)
            xres[f] = jnp.where(second, out, x).astype(jnp.bfloat16)
            ssum[0] += fold(out)
            ssum[1] += fold(out * out)

        return [functools.partial(one, f) for f in range(c * CHUNK, (c + 1) * CHUNK)]

    for copy in small_copies:
        copy.wait()
    for i in range(3):
        for layer in range(LAYERS):
            params[i, layer] = small[i, layer : layer + 1, :]
    with jax.named_scope("entry_wait"):
        pl.semaphore_wait(barrier, n_hp * n_cp - 1)
    with jax.named_scope("send_sums"):
        send_sums(0)
    start_times(0)
    for c in range(n_chunks):
        start_rows(0, c)

    def layer_body(layer, _):
        slot = lax.rem(layer, 2)
        other = 1 - slot
        more = layer < LAYERS - 1

        @pl.when(more)
        def _():
            start_weights(layer + 1, other)

        with jax.named_scope("statistics"):
            statistics(layer)

        with jax.named_scope("act_own"):
            @pl.when(has_prev)
            def _():
                time_copy(slot, 0).wait_recv()

            @pl.loop(0, OWN + 2)
            def _(f):
                activate(slot, 1, f)

        with jax.named_scope("w_wait"):
            for k, di in slab_order:
                weight_copy(layer, slot, k, di).wait()

        own_act = [functools.partial(activate, slot, 1, f) for f in range(OWN + 2, frames + 2)]
        with jax.named_scope("own0"):
            for start in range(0, frames - OWN, OWN):
                acc[start : start + OWN] = taps(slot, (1,), start, OWN, own_act[start : start + OWN])
        with jax.named_scope("halo_wait0"):
            halo_wait(slot, 0)
        with jax.named_scope("own1"):
            acc[frames - OWN : frames] = taps(slot, (1,), frames - OWN, OWN, halo_act(slot, 0))
        ssum[...] = jnp.zeros_like(ssum)
        for pair in range(n_chunks // 2):
            chunks = (2 * pair, 2 * pair + 1)
            with jax.named_scope(f"halo_wait{pair + 1}"):
                for c in chunks:
                    if c < n_chunks - 1:
                        halo_wait(slot, c + 1)
            with jax.named_scope(f"chunks{pair}"):
                for c in chunks:
                    side = finish(layer, other, c - 1) if c > 0 else []
                    side += halo_act(slot, c + 1) if c < n_chunks - 1 else []
                    acc[c * CHUNK : (c + 1) * CHUNK] += taps(slot, (0, 2), c * CHUNK, CHUNK, side)
            if pair == 0:
                @pl.when(more)
                def _():
                    start_rows(other, 0)

        with jax.named_scope("send_wait"):
            wait_sends(slot)
        with jax.named_scope("finish"):
            for work in finish(layer, other, n_chunks - 1):
                work()

        @pl.when(more)
        def _():
            with jax.named_scope("send_sums"):
                send_sums(layer + 1)
            with jax.named_scope("send_rest"):
                start_times(other)
                for c in range(1, n_chunks):
                    start_rows(other, c)

        return 0

    lax.fori_loop(0, LAYERS, layer_body, 0)

    @pl.loop(0, frames)
    def _(f):
        o_ref[f] = xres[f]


def solution(mesh):
    n_hp, n_cp = mesh.shape["hp"], mesh.shape["cp"]

    def local_decode(lat, conv_w, conv_b, gn_gamma, gn_beta):
        frames, rows, width, channels = lat.shape
        n_chunks = frames // CHUNK
        total_count = float(frames * n_cp * rows * n_hp * width * (channels // GROUPS))
        hbm_spec = pl.BlockSpec(memory_space=pltpu.HBM)
        vmem_spec = pl.BlockSpec(memory_space=pltpu.VMEM)
        bf16, f32 = jnp.bfloat16, jnp.float32
        flops = LAYERS * 2 * frames * width * 27 * channels * channels
        out = pl.pallas_call(
            functools.partial(decode_kernel, n_hp, n_cp, total_count),
            out_shape=jax.ShapeDtypeStruct((frames, width, channels), bf16),
            in_specs=[hbm_spec] * 5,
            out_specs=vmem_spec,
            scratch_shapes=[
                pltpu.VMEM((2, 9, 3 * channels, channels), bf16),
                pltpu.VMEM((2, 3, frames + 2, width, channels), bf16),
                pltpu.VMEM((3, frames + 2, width, 3 * channels), bf16),
                pltpu.VMEM((frames, width, channels), f32),
                pltpu.VMEM((frames, width, channels), bf16),
                pltpu.VMEM((3, LAYERS, channels), f32),
                pltpu.VMEM((3, LAYERS, 1, channels), f32),
                pltpu.VMEM((2, 8, channels), f32),
                pltpu.VMEM((8, 128), f32),
                pltpu.VMEM((3, 8, channels), f32),
                pltpu.VMEM((LAYERS, 1, 128), f32),
                pltpu.VMEM((LAYERS, n_hp * n_cp, 1, 128), f32),
                pltpu.SemaphoreType.DMA((2, 9)),
                pltpu.SemaphoreType.DMA((2,)),
                pltpu.SemaphoreType.DMA((3,)),
                pltpu.SemaphoreType.DMA((2, 3, n_chunks + 1)),
                pltpu.SemaphoreType.DMA((2, 3, n_chunks + 1)),
                pltpu.SemaphoreType.DMA((LAYERS,)),
                pltpu.SemaphoreType.DMA((LAYERS,)),
            ],
            compiler_params=pltpu.CompilerParams(
                collective_id=0, has_side_effects=True, vmem_limit_bytes=60 * 1024 * 1024),
            cost_estimate=pl.CostEstimate(flops=flops, bytes_accessed=conv_w.size * 2, transcendentals=0),
        )(lat.reshape(frames, width, channels), conv_w.reshape(LAYERS, 9, 3 * channels, channels),
          conv_b, gn_gamma, gn_beta)
        return out.reshape(lat.shape)

    video_spec = P(("dp", "cp"), "hp", None, None)
    return jax.shard_map(local_decode, mesh=mesh, in_specs=(video_spec, P(), P(), P(), P()), out_specs=video_spec, check_vma=False)
```

```python
import functools

import jax
import jax.numpy as jnp
from jax import lax
from jax.experimental import pallas as pl
from jax.experimental.pallas import tpu as pltpu
from jax.sharding import PartitionSpec as P

GROUPS = 32
EPS = 1e-6
LAYERS = 4
MESH = pl.DeviceIdType.MESH
CHUNK = 3


def lane_sums(y, lane):
    for s in (1, 4):
        place = (lane // s) & 3
        total = y
        for d in (-3, -2, -1, 1, 2, 3):
            inside = jnp.logical_and(place + d >= 0, place + d <= 3)
            total = total + jnp.where(inside, pltpu.roll(y, (-d * s) % 128, 1), 0.0)
        y = total
    return y


def tree_sum(terms):
    while len(terms) > 1:
        terms = [a + b for a, b in zip(terms[::2], terms[1::2])] + terms[len(terms) & ~1 :]
    return terms[0]


def decode_kernel(n_hp, n_cp, total_count, lat_ref, w_ref, b_ref, g_ref, be_ref, o_ref,
                  wbuf, raw, act, acc, xres, small, params, ssum, st8, coef, msg, peers,
                  w_sem, lat_sem, small_sem, out_sem, send_sem, recv_sem, msg_send, msg_recv):
    frames, width, channels = xres.shape
    n_chunks = frames // CHUNK
    hp = lax.axis_index("hp")
    cp = lax.axis_index("cp")
    has_up = hp > 0
    has_down = hp < n_hp - 1
    has_next = cp < n_cp - 1
    has_prev = cp > 0

    slab_order = [(k, 1) for k in range(3)] + [(k, di) for di in (0, 2) for k in range(3)]

    def weight_copy(layer, slot, k, di):
        slab = k * 3 + di
        return pltpu.make_async_copy(w_ref.at[layer, slab], wbuf.at[slot, slab], w_sem.at[slot, slab])

    def start_weights(layer, slot):
        for k, di in slab_order:
            weight_copy(layer, slot, k, di).start()

    lat_copies = [pltpu.make_async_copy(lat_ref, raw.at[0, 1, pl.ds(2, frames)], lat_sem.at[0]),
                  pltpu.make_async_copy(lat_ref, xres, lat_sem.at[1])]
    small_copies = [pltpu.make_async_copy(ref, small.at[i], small_sem.at[i]) for i, ref in enumerate((b_ref, g_ref, be_ref))]
    for copy in lat_copies + small_copies:
        copy.start()

    def others(visit):
        @pl.loop(0, n_hp)
        def _(i):
            for j in range(n_cp):
                target = {"hp": lax.rem(hp + n_hp // 2 + i, n_hp), "cp": lax.rem(cp + n_cp // 2 + j, n_cp)}
                if j == n_cp // 2:
                    pl.when(i != n_hp // 2)(functools.partial(visit, target))
                else:
                    visit(target)

    barrier = pltpu.get_barrier_semaphore()
    with jax.named_scope("entry_signals"):
        others(lambda target: pl.semaphore_signal(barrier, inc=1, device_id=target, device_id_type=MESH))

    def row_copy(slot, c, to_down):
        span = pl.ds(2 + c * CHUNK, CHUNK)
        row = 0 if to_down else 2
        return pltpu.make_async_remote_copy(
            src_ref=raw.at[slot, 1, span], dst_ref=raw.at[slot, row, span],
            send_sem=send_sem.at[slot, row, c], recv_sem=recv_sem.at[slot, row, c],
            device_id={"hp": hp + (1 if to_down else -1)}, device_id_type=MESH)

    def time_copy(slot, dh):
        row = dh if dh is None else (0 if dh == 1 else 2)
        row = 1 if dh == 0 else row
        return pltpu.make_async_remote_copy(
            src_ref=raw.at[slot, 1, pl.ds(frames, 2)], dst_ref=raw.at[slot, row, pl.ds(0, 2)],
            send_sem=send_sem.at[slot, row, n_chunks], recv_sem=recv_sem.at[slot, row, n_chunks],
            device_id={"hp": hp + dh, "cp": cp + 1}, device_id_type=MESH)

    def start_rows(slot, c):
        @pl.when(has_up)
        def _():
            row_copy(slot, c, False).start()

        @pl.when(has_down)
        def _():
            row_copy(slot, c, True).start()

    def start_times(slot):
        @pl.when(has_next)
        def _():
            time_copy(slot, 0).start()

        @pl.when(jnp.logical_and(has_next, has_up))
        def _():
            time_copy(slot, -1).start()

        @pl.when(jnp.logical_and(has_next, has_down))
        def _():
            time_copy(slot, 1).start()

    def wait_sends(slot):
        for c in range(n_chunks):
            @pl.when(has_up)
            def _():
                row_copy(slot, c, False).wait_send()

            @pl.when(has_down)
            def _():
                row_copy(slot, c, True).wait_send()

        @pl.when(has_next)
        def _():
            time_copy(slot, 0).wait_send()

        @pl.when(jnp.logical_and(has_next, has_up))
        def _():
            time_copy(slot, -1).wait_send()

        @pl.when(jnp.logical_and(has_next, has_down))
        def _():
            time_copy(slot, 1).wait_send()

    for row, ok in ((0, has_up), (2, has_down)):
        @pl.when(jnp.logical_not(ok))
        def _():
            @pl.loop(0, frames + 2)
            def _(f):
                for slot in range(2):
                    raw[slot, row, f] = jnp.zeros((width, channels), jnp.bfloat16)

    @pl.when(jnp.logical_not(has_prev))
    def _():
        for slot in range(2):
            for row in range(3):
                for f in range(2):
                    raw[slot, row, f] = jnp.zeros((width, channels), jnp.bfloat16)

    with jax.named_scope("lat_wait"):
        for copy in lat_copies:
            copy.wait()
    start_weights(0, 0)

    def fold(v):
        return jnp.sum(v.reshape(-1, 8, v.shape[-1]), axis=0)

    ssum[...] = jnp.zeros_like(ssum)

    @pl.loop(0, frames)
    def _(f):
        v = xres[f].astype(jnp.float32)
        ssum[0] += fold(v)
        ssum[1] += fold(v * v)

    lane = lax.broadcasted_iota(jnp.int32, (8, 128), 1)
    sub = lax.broadcasted_iota(jnp.int32, (8, 128), 0)
    pick = (lane & 15) == sub

    me = hp * n_cp + cp

    def send_sums(layer):
        for s in range(2):
            for i in range(4):
                st8[s * 4 + i : s * 4 + i + 1, :] = jnp.sum(ssum[s, :, i * 128 : (i + 1) * 128], axis=0, keepdims=True)
        mine = jnp.where(pick, lane_sums(st8[...], lane), 0.0)
        msg[layer] = jnp.sum(mine, axis=0, keepdims=True)
        peers[layer, me] = msg[layer]
        others(lambda target: pltpu.make_async_remote_copy(
            src_ref=msg.at[layer], dst_ref=peers.at[layer, me], send_sem=msg_send.at[layer], recv_sem=msg_recv.at[layer],
            device_id=target, device_id_type=MESH).start())

    def statistics(layer):
        rest = peers.at[layer, pl.ds(0, n_hp * n_cp - 1)]
        pltpu.make_async_copy(rest, rest, msg_recv.at[layer]).wait()
        pltpu.make_async_copy(rest, rest, msg_send.at[layer]).wait()
        total = tree_sum([peers[layer, i] for i in range(n_hp * n_cp)])
        st8[...] = lane_sums(jnp.where(pick, jnp.broadcast_to(total, (8, 128)), 0.0), lane)
        mean = st8[0:4, :] * (1.0 / total_count)
        var = st8[4:8, :] * (1.0 / total_count) - mean * mean
        inv = lax.rsqrt(var + EPS)
        st8[0:4, :] = inv
        st8[4:8, :] = mean * inv
        for i in range(4):
            lanes = slice(i * 128, (i + 1) * 128)
            gamma = 0.5 * params[1, layer, :, lanes]
            scale = gamma * st8[i : i + 1, :]
            shift = 0.5 * params[2, layer, :, lanes] - st8[4 + i : 5 + i, :] * gamma
            for row, ok in ((0, has_up), (1, None), (2, has_down)):
                coef[row, 0:1, lanes] = scale if ok is None else jnp.where(ok, scale, 0.0)
                coef[row, 1:2, lanes] = shift if ok is None else jnp.where(ok, shift, 0.0)

    first_frame = jnp.where(has_prev, 0, 2)
    col = lax.broadcasted_iota(jnp.int32, (width, channels), 0)

    def activate(slot, row, f):
        v = raw[slot, row, jnp.maximum(f, first_frame)].astype(jnp.float32)
        u = v * coef[row, 0:1, :] + coef[row, 1:2, :]
        y = u * jnp.tanh(u) + u
        left = jnp.where(col == 0, 0.0, pltpu.roll(y, 1, 0))
        right = jnp.where(col == width - 1, 0.0, pltpu.roll(y, width - 1, 0))
        for dj, v in enumerate((left, y, right)):
            act[row, f, :, dj * channels : (dj + 1) * channels] = v.astype(jnp.bfloat16)

    def halo_wait(slot, c):
        for row, ok in ((0, has_up), (2, has_down)):
            if c == 0:
                @pl.when(jnp.logical_and(ok, has_prev))
                def _():
                    time_copy(slot, 1 if row == 0 else -1).wait_recv()

            @pl.when(ok)
            def _():
                row_copy(slot, c, row == 0).wait_recv()

    def halo_act(slot, c):
        frames_in = range(2 + c * CHUNK if c else 0, 2 + (c + 1) * CHUNK)
        return [functools.partial(activate, slot, row, f) for f in frames_in for row in (0, 2)]

    def conv_chunk(slot, c, side):
        total = None
        for d in (1, 0, 2):
            for k in range(3):
                if d == 1 and c == 0:
                    for f in range(2 + k if k else 0, 3 + k):
                        activate(slot, 1, f)
                lhs = act[d, c * CHUNK + k : c * CHUNK + k + CHUNK].reshape(CHUNK * width, 3 * channels)
                part = jnp.dot(lhs, wbuf[slot, k * 3 + d], preferred_element_type=jnp.float32)
                total = part if total is None else total + part
                if d == 1:
                    for work in side[len(side) * k // 3 : len(side) * (k + 1) // 3]:
                        work()
        if c < n_chunks - 1:
            for f in range((c + 1) * CHUNK + 2, (c + 2) * CHUNK + 2):
                activate(slot, 1, f)
        acc[c * CHUNK : (c + 1) * CHUNK] = total.reshape(CHUNK, width, channels)

    def finish(layer, other, c):
        second = lax.rem(layer, 2) == 1

        def one(f):
            h = (acc[f] + params[0, layer]).astype(jnp.bfloat16).astype(jnp.float32)
            x = xres[f].astype(jnp.float32)
            out = (h + jnp.where(second, x, 0.0)).astype(jnp.bfloat16)
            raw[other, 1, 2 + f] = out
            out = out.astype(jnp.float32)
            xres[f] = jnp.where(second, out, x).astype(jnp.bfloat16)
            ssum[0] += fold(out)
            ssum[1] += fold(out * out)

        return [functools.partial(one, f) for f in range(c * CHUNK, (c + 1) * CHUNK)]

    for copy in small_copies:
        copy.wait()
    for i in range(3):
        for layer in range(LAYERS):
            params[i, layer] = small[i, layer : layer + 1, :]
    with jax.named_scope("entry_wait"):
        pl.semaphore_wait(barrier, n_hp * n_cp - 1)
    with jax.named_scope("send_sums"):
        send_sums(0)
    start_times(0)
    for c in range(n_chunks):
        start_rows(0, c)

    def out_copy(c):
        span = pl.ds(c * CHUNK, CHUNK)
        return pltpu.make_async_copy(xres.at[span], o_ref.at[span], out_sem.at[c])

    def layer_body(layer, _):
        slot = lax.rem(layer, 2)
        other = 1 - slot
        more = layer < LAYERS - 1

        @pl.when(more)
        def _():
            start_weights(layer + 1, other)

        with jax.named_scope("statistics"):
            statistics(layer)

        with jax.named_scope("w_wait"):
            @pl.when(has_prev)
            def _():
                time_copy(slot, 0).wait_recv()

            for k, di in slab_order:
                weight_copy(layer, slot, k, di).wait()

        ssum[...] = jnp.zeros_like(ssum)
        for c in range(n_chunks):
            with jax.named_scope(f"halo_wait{c}"):
                halo_wait(slot, c)
            with jax.named_scope(f"chunk{c}"):
                side = finish(layer, other, c - 1) if c > 0 else []
                conv_chunk(slot, c, side + halo_act(slot, c))

            if 0 < c < n_chunks - 1:
                @pl.when(more)
                def _():
                    start_rows(other, c - 1)

                @pl.when(jnp.logical_not(more))
                def _():
                    out_copy(c - 1).start()

        with jax.named_scope("send_wait"):
            wait_sends(slot)
        with jax.named_scope("finish"):
            for work in finish(layer, other, n_chunks - 1):
                work()

        @pl.when(more)
        def _():
            with jax.named_scope("send_sums"):
                send_sums(layer + 1)
            with jax.named_scope("send_rest"):
                start_times(other)
                for c in range(2, n_chunks):
                    start_rows(other, c)

        return 0

    lax.fori_loop(0, LAYERS, layer_body, 0)

    for c in range(2, n_chunks):
        out_copy(c).start()
    for c in range(n_chunks):
        out_copy(c).wait()


def solution(mesh):
    n_hp, n_cp = mesh.shape["hp"], mesh.shape["cp"]

    def local_decode(lat, conv_w, conv_b, gn_gamma, gn_beta):
        frames, rows, width, channels = lat.shape
        n_chunks = frames // CHUNK
        total_count = float(frames * n_cp * rows * n_hp * width * (channels // GROUPS))
        hbm_spec = pl.BlockSpec(memory_space=pltpu.HBM)
        bf16, f32 = jnp.bfloat16, jnp.float32
        flops = LAYERS * 2 * frames * width * 27 * channels * channels
        out = pl.pallas_call(
            functools.partial(decode_kernel, n_hp, n_cp, total_count),
            out_shape=jax.ShapeDtypeStruct((frames, width, channels), bf16),
            in_specs=[hbm_spec] * 5,
            out_specs=hbm_spec,
            scratch_shapes=[
                pltpu.VMEM((2, 9, 3 * channels, channels), bf16),
                pltpu.VMEM((2, 3, frames + 2, width, channels), bf16),
                pltpu.VMEM((3, frames + 2, width, 3 * channels), bf16),
                pltpu.VMEM((frames, width, channels), f32),
                pltpu.VMEM((frames, width, channels), bf16),
                pltpu.VMEM((3, LAYERS, channels), f32),
                pltpu.VMEM((3, LAYERS, 1, channels), f32),
                pltpu.VMEM((2, 8, channels), f32),
                pltpu.VMEM((8, 128), f32),
                pltpu.VMEM((3, 8, channels), f32),
                pltpu.VMEM((LAYERS, 1, 128), f32),
                pltpu.VMEM((LAYERS, n_hp * n_cp, 1, 128), f32),
                pltpu.SemaphoreType.DMA((2, 9)),
                pltpu.SemaphoreType.DMA((2,)),
                pltpu.SemaphoreType.DMA((3,)),
                pltpu.SemaphoreType.DMA((n_chunks,)),
                pltpu.SemaphoreType.DMA((2, 3, n_chunks + 1)),
                pltpu.SemaphoreType.DMA((2, 3, n_chunks + 1)),
                pltpu.SemaphoreType.DMA((LAYERS,)),
                pltpu.SemaphoreType.DMA((LAYERS,)),
            ],
            compiler_params=pltpu.CompilerParams(
                collective_id=0, has_side_effects=True, vmem_limit_bytes=60 * 1024 * 1024),
            cost_estimate=pl.CostEstimate(flops=flops, bytes_accessed=conv_w.size * 2, transcendentals=0),
        )(lat.reshape(frames, width, channels), conv_w.reshape(LAYERS, 9, 3 * channels, channels),
          conv_b, gn_gamma, gn_beta)
        return out.reshape(lat.shape)

    video_spec = P(("dp", "cp"), "hp", None, None)
    return jax.shard_map(local_decode, mesh=mesh, in_specs=(video_spec, P(), P(), P(), P()), out_specs=video_spec, check_vma=False)
```

```python
import functools

import jax
import jax.numpy as jnp
from jax import lax
from jax.experimental import pallas as pl
from jax.experimental.pallas import tpu as pltpu
from jax.sharding import PartitionSpec as P

GROUPS = 32
EPS = 1e-6
LAYERS = 4
MESH = pl.DeviceIdType.MESH
CHUNK = 3


def lane_sums(y, lane):
    for s in (1, 4):
        place = (lane // s) & 3
        total = y
        for d in (-3, -2, -1, 1, 2, 3):
            inside = jnp.logical_and(place + d >= 0, place + d <= 3)
            total = total + jnp.where(inside, pltpu.roll(y, (-d * s) % 128, 1), 0.0)
        y = total
    return y


def tree_sum(terms):
    while len(terms) > 1:
        terms = [a + b for a, b in zip(terms[::2], terms[1::2])] + terms[len(terms) & ~1 :]
    return terms[0]


def decode_kernel(n_hp, n_cp, total_count, lat_ref, w_ref, b_ref, g_ref, be_ref, o_ref,
                  wbuf, raw, act, acc, xres, small, params, ssum, st8, coef, msg, peers,
                  w_sem, lat_sem, small_sem, out_sem, send_sem, recv_sem, msg_send, msg_recv):
    frames, width, channels = xres.shape
    n_chunks = frames // CHUNK
    hp = lax.axis_index("hp")
    cp = lax.axis_index("cp")
    has_up = hp > 0
    has_down = hp < n_hp - 1
    has_next = cp < n_cp - 1
    has_prev = cp > 0

    slab_order = [(k, 1) for k in range(3)] + [(k, di) for di in (0, 2) for k in range(3)]

    def weight_copy(layer, slot, k, di):
        slab = k * 3 + di
        return pltpu.make_async_copy(w_ref.at[layer, slab], wbuf.at[slot, slab], w_sem.at[slot, slab])

    def start_weights(layer, slot):
        for k, di in slab_order:
            weight_copy(layer, slot, k, di).start()

    lat_copies = [pltpu.make_async_copy(lat_ref, raw.at[0, 1, pl.ds(2, frames)], lat_sem.at[0]),
                  pltpu.make_async_copy(lat_ref, xres, lat_sem.at[1])]
    small_copies = [pltpu.make_async_copy(ref, small.at[i], small_sem.at[i]) for i, ref in enumerate((b_ref, g_ref, be_ref))]
    for copy in lat_copies + small_copies:
        copy.start()

    def others(visit):
        @pl.loop(0, n_hp)
        def _(i):
            for j in range(n_cp):
                target = {"hp": lax.rem(hp + n_hp // 2 + i, n_hp), "cp": lax.rem(cp + n_cp // 2 + j, n_cp)}
                if j == n_cp // 2:
                    pl.when(i != n_hp // 2)(functools.partial(visit, target))
                else:
                    visit(target)

    barrier = pltpu.get_barrier_semaphore()
    with jax.named_scope("entry_signals"):
        others(lambda target: pl.semaphore_signal(barrier, inc=1, device_id=target, device_id_type=MESH))

    def row_copy(slot, c, to_down):
        span = pl.ds(2 + c * CHUNK, CHUNK)
        row = 0 if to_down else 2
        return pltpu.make_async_remote_copy(
            src_ref=raw.at[slot, 1, span], dst_ref=raw.at[slot, row, span],
            send_sem=send_sem.at[slot, row, c], recv_sem=recv_sem.at[slot, row, c],
            device_id={"hp": hp + (1 if to_down else -1)}, device_id_type=MESH)

    def time_copy(slot, dh):
        row = dh if dh is None else (0 if dh == 1 else 2)
        row = 1 if dh == 0 else row
        return pltpu.make_async_remote_copy(
            src_ref=raw.at[slot, 1, pl.ds(frames, 2)], dst_ref=raw.at[slot, row, pl.ds(0, 2)],
            send_sem=send_sem.at[slot, row, n_chunks], recv_sem=recv_sem.at[slot, row, n_chunks],
            device_id={"hp": hp + dh, "cp": cp + 1}, device_id_type=MESH)

    def start_rows(slot, c):
        @pl.when(has_up)
        def _():
            row_copy(slot, c, False).start()

        @pl.when(has_down)
        def _():
            row_copy(slot, c, True).start()

    def start_times(slot):
        @pl.when(has_next)
        def _():
            time_copy(slot, 0).start()

        @pl.when(jnp.logical_and(has_next, has_up))
        def _():
            time_copy(slot, -1).start()

        @pl.when(jnp.logical_and(has_next, has_down))
        def _():
            time_copy(slot, 1).start()

    def wait_sends(slot):
        for c in range(n_chunks):
            @pl.when(has_up)
            def _():
                row_copy(slot, c, False).wait_send()

            @pl.when(has_down)
            def _():
                row_copy(slot, c, True).wait_send()

        @pl.when(has_next)
        def _():
            time_copy(slot, 0).wait_send()

        @pl.when(jnp.logical_and(has_next, has_up))
        def _():
            time_copy(slot, -1).wait_send()

        @pl.when(jnp.logical_and(has_next, has_down))
        def _():
            time_copy(slot, 1).wait_send()

    for row, ok in ((0, has_up), (2, has_down)):
        @pl.when(jnp.logical_not(ok))
        def _():
            @pl.loop(0, frames + 2)
            def _(f):
                for slot in range(2):
                    raw[slot, row, f] = jnp.zeros((width, channels), jnp.bfloat16)

    @pl.when(jnp.logical_not(has_prev))
    def _():
        for slot in range(2):
            for row in range(3):
                for f in range(2):
                    raw[slot, row, f] = jnp.zeros((width, channels), jnp.bfloat16)

    with jax.named_scope("lat_wait"):
        for copy in lat_copies:
            copy.wait()
    start_weights(0, 0)

    def fold(v):
        return jnp.sum(v.reshape(-1, 8, v.shape[-1]), axis=0)

    ssum[...] = jnp.zeros_like(ssum)

    @pl.loop(0, frames)
    def _(f):
        v = xres[f].astype(jnp.float32)
        ssum[0] += fold(v)
        ssum[1] += fold(v * v)

    lane = lax.broadcasted_iota(jnp.int32, (8, 128), 1)
    sub = lax.broadcasted_iota(jnp.int32, (8, 128), 0)
    pick = (lane & 15) == sub

    me = hp * n_cp + cp

    def send_sums(layer):
        for s in range(2):
            for i in range(4):
                st8[s * 4 + i : s * 4 + i + 1, :] = jnp.sum(ssum[s, :, i * 128 : (i + 1) * 128], axis=0, keepdims=True)
        mine = jnp.where(pick, lane_sums(st8[...], lane), 0.0)
        msg[layer] = jnp.sum(mine, axis=0, keepdims=True)
        peers[layer, me] = msg[layer]
        others(lambda target: pltpu.make_async_remote_copy(
            src_ref=msg.at[layer], dst_ref=peers.at[layer, me], send_sem=msg_send.at[layer], recv_sem=msg_recv.at[layer],
            device_id=target, device_id_type=MESH).start())

    def statistics(layer):
        rest = peers.at[layer, pl.ds(0, n_hp * n_cp - 1)]
        pltpu.make_async_copy(rest, rest, msg_recv.at[layer]).wait()
        pltpu.make_async_copy(rest, rest, msg_send.at[layer]).wait()
        total = tree_sum([peers[layer, i] for i in range(n_hp * n_cp)])
        st8[...] = lane_sums(jnp.where(pick, jnp.broadcast_to(total, (8, 128)), 0.0), lane)
        mean = st8[0:4, :] * (1.0 / total_count)
        var = st8[4:8, :] * (1.0 / total_count) - mean * mean
        inv = lax.rsqrt(var + EPS)
        st8[0:4, :] = inv
        st8[4:8, :] = mean * inv
        for i in range(4):
            lanes = slice(i * 128, (i + 1) * 128)
            gamma = 0.5 * params[1, layer, :, lanes]
            scale = gamma * st8[i : i + 1, :]
            shift = 0.5 * params[2, layer, :, lanes] - st8[4 + i : 5 + i, :] * gamma
            for row, ok in ((0, has_up), (1, None), (2, has_down)):
                coef[row, 0:1, lanes] = scale if ok is None else jnp.where(ok, scale, 0.0)
                coef[row, 1:2, lanes] = shift if ok is None else jnp.where(ok, shift, 0.0)

    first_frame = jnp.where(has_prev, 0, 2)
    col = lax.broadcasted_iota(jnp.int32, (width, channels), 0)

    def activate(slot, row, f):
        v = raw[slot, row, jnp.maximum(f, first_frame)].astype(jnp.float32)
        u = v * coef[row, 0:1, :] + coef[row, 1:2, :]
        y = u * jnp.tanh(u) + u
        left = jnp.where(col == 0, 0.0, pltpu.roll(y, 1, 0))
        right = jnp.where(col == width - 1, 0.0, pltpu.roll(y, width - 1, 0))
        for dj, v in enumerate((left, y, right)):
            act[row, f, :, dj * channels : (dj + 1) * channels] = v.astype(jnp.bfloat16)

    def halo_wait(slot, c):
        for row, ok in ((0, has_up), (2, has_down)):
            if c == 0:
                @pl.when(jnp.logical_and(ok, has_prev))
                def _():
                    time_copy(slot, 1 if row == 0 else -1).wait_recv()

            @pl.when(ok)
            def _():
                row_copy(slot, c, row == 0).wait_recv()

    def halo_act(slot, c):
        frames_in = range(2 + c * CHUNK if c else 0, 2 + (c + 1) * CHUNK)
        return [functools.partial(activate, slot, row, f) for f in frames_in for row in (0, 2)]

    def conv_chunk(slot, c, side):
        total = None
        for f in range(c * CHUNK + 2 if c else 0, c * CHUNK + 5):
            activate(slot, 1, f)
        for d in (1, 0, 2):
            for k in range(3):
                lhs = act[d, c * CHUNK + k : c * CHUNK + k + CHUNK].reshape(CHUNK * width, 3 * channels)
                part = jnp.dot(lhs, wbuf[slot, k * 3 + d], preferred_element_type=jnp.float32)
                total = part if total is None else total + part
                if d == 1:
                    for work in side[len(side) * k // 3 : len(side) * (k + 1) // 3]:
                        work()
        return total.reshape(CHUNK, width, channels)

    def finish(layer, other, c, y=None):
        second = lax.rem(layer, 2) == 1

        def one(f):
            h = acc[f - c * CHUNK] if y is None else y[f - c * CHUNK]
            h = (h + params[0, layer]).astype(jnp.bfloat16).astype(jnp.float32)
            x = xres[f].astype(jnp.float32)
            out = (h + jnp.where(second, x, 0.0)).astype(jnp.bfloat16)
            raw[other, 1, 2 + f] = out
            out = out.astype(jnp.float32)
            xres[f] = jnp.where(second, out, x).astype(jnp.bfloat16)
            ssum[0] += fold(out)
            ssum[1] += fold(out * out)

        return [functools.partial(one, f) for f in range(c * CHUNK, (c + 1) * CHUNK)]

    for copy in small_copies:
        copy.wait()
    for i in range(3):
        for layer in range(LAYERS):
            params[i, layer] = small[i, layer : layer + 1, :]
    with jax.named_scope("entry_wait"):
        pl.semaphore_wait(barrier, n_hp * n_cp - 1)
    with jax.named_scope("send_sums"):
        send_sums(0)
    start_times(0)
    for c in range(n_chunks):
        start_rows(0, c)

    def out_copy(c):
        span = pl.ds(c * CHUNK, CHUNK)
        return pltpu.make_async_copy(xres.at[span], o_ref.at[span], out_sem.at[c])

    def layer_body(layer, _):
        slot = lax.rem(layer, 2)
        other = 1 - slot
        more = layer < LAYERS - 1

        @pl.when(more)
        def _():
            start_weights(layer + 1, other)

        with jax.named_scope("statistics"):
            statistics(layer)

        @pl.when(layer > 0)
        def _():
            for c in range(2, n_chunks):
                start_rows(slot, c)

        with jax.named_scope("w_wait"):
            @pl.when(has_prev)
            def _():
                time_copy(slot, 0).wait_recv()

            for k, di in slab_order:
                weight_copy(layer, slot, k, di).wait()

        ssum[...] = jnp.zeros_like(ssum)
        for c in range(n_chunks):
            with jax.named_scope(f"halo_wait{c}"):
                halo_wait(slot, c)
            with jax.named_scope(f"chunk{c}"):
                side = finish(layer, other, c - 1) if c == n_chunks - 1 else []
                y = conv_chunk(slot, c, side + halo_act(slot, c))
                if c == n_chunks - 2:
                    acc[...] = y
                else:
                    for work in finish(layer, other, c, y):
                        work()

            if c < 2:
                @pl.when(more)
                def _():
                    start_rows(other, c)

                @pl.when(jnp.logical_not(more))
                def _():
                    out_copy(c).start()

        with jax.named_scope("send_wait"):
            wait_sends(slot)
        @pl.when(more)
        def _():
            with jax.named_scope("send_sums"):
                send_sums(layer + 1)
            with jax.named_scope("send_rest"):
                start_times(other)

        return 0

    lax.fori_loop(0, LAYERS, layer_body, 0)

    for c in range(2, n_chunks):
        out_copy(c).start()
    for c in range(n_chunks):
        out_copy(c).wait()


def solution(mesh):
    n_hp, n_cp = mesh.shape["hp"], mesh.shape["cp"]

    def local_decode(lat, conv_w, conv_b, gn_gamma, gn_beta):
        frames, rows, width, channels = lat.shape
        n_chunks = frames // CHUNK
        total_count = float(frames * n_cp * rows * n_hp * width * (channels // GROUPS))
        hbm_spec = pl.BlockSpec(memory_space=pltpu.HBM)
        bf16, f32 = jnp.bfloat16, jnp.float32
        flops = LAYERS * 2 * frames * width * 27 * channels * channels
        out = pl.pallas_call(
            functools.partial(decode_kernel, n_hp, n_cp, total_count),
            out_shape=jax.ShapeDtypeStruct((frames, width, channels), bf16),
            in_specs=[hbm_spec] * 5,
            out_specs=hbm_spec,
            scratch_shapes=[
                pltpu.VMEM((2, 9, 3 * channels, channels), bf16),
                pltpu.VMEM((2, 3, frames + 2, width, channels), bf16),
                pltpu.VMEM((3, frames + 2, width, 3 * channels), bf16),
                pltpu.VMEM((CHUNK, width, channels), f32),
                pltpu.VMEM((frames, width, channels), bf16),
                pltpu.VMEM((3, LAYERS, channels), f32),
                pltpu.VMEM((3, LAYERS, 1, channels), f32),
                pltpu.VMEM((2, 8, channels), f32),
                pltpu.VMEM((8, 128), f32),
                pltpu.VMEM((3, 8, channels), f32),
                pltpu.VMEM((LAYERS, 1, 128), f32),
                pltpu.VMEM((LAYERS, n_hp * n_cp, 1, 128), f32),
                pltpu.SemaphoreType.DMA((2, 9)),
                pltpu.SemaphoreType.DMA((2,)),
                pltpu.SemaphoreType.DMA((3,)),
                pltpu.SemaphoreType.DMA((n_chunks,)),
                pltpu.SemaphoreType.DMA((2, 3, n_chunks + 1)),
                pltpu.SemaphoreType.DMA((2, 3, n_chunks + 1)),
                pltpu.SemaphoreType.DMA((LAYERS,)),
                pltpu.SemaphoreType.DMA((LAYERS,)),
            ],
            compiler_params=pltpu.CompilerParams(
                collective_id=0, has_side_effects=True, vmem_limit_bytes=60 * 1024 * 1024),
            cost_estimate=pl.CostEstimate(flops=flops, bytes_accessed=conv_w.size * 2, transcendentals=0),
        )(lat.reshape(frames, width, channels), conv_w.reshape(LAYERS, 9, 3 * channels, channels),
          conv_b, gn_gamma, gn_beta)
        return out.reshape(lat.shape)

    video_spec = P(("dp", "cp"), "hp", None, None)
    return jax.shard_map(local_decode, mesh=mesh, in_specs=(video_spec, P(), P(), P(), P()), out_specs=video_spec, check_vma=False)
```

```python
import functools

import jax
import jax.numpy as jnp
from jax import lax
from jax.experimental import pallas as pl
from jax.experimental.pallas import tpu as pltpu
from jax.sharding import PartitionSpec as P

GROUPS = 32
EPS = 1e-6
LAYERS = 4
MESH = pl.DeviceIdType.MESH
CHUNK = 3


def lane_sums(y, lane):
    for s in (1, 4):
        place = (lane // s) & 3
        total = y
        for d in (-3, -2, -1, 1, 2, 3):
            inside = jnp.logical_and(place + d >= 0, place + d <= 3)
            total = total + jnp.where(inside, pltpu.roll(y, (-d * s) % 128, 1), 0.0)
        y = total
    return y


def tree_sum(terms):
    while len(terms) > 1:
        terms = [a + b for a, b in zip(terms[::2], terms[1::2])] + terms[len(terms) & ~1 :]
    return terms[0]


def decode_kernel(n_hp, n_cp, total_count, lat_ref, w_ref, b_ref, g_ref, be_ref, o_ref,
                  wbuf, raw, act, xres, small, params, ssum, st8, coef, msg, peers,
                  w_sem, lat_sem, small_sem, send_sem, recv_sem, msg_send, msg_recv):
    frames, width, channels = xres.shape
    n_chunks = frames // CHUNK
    hp = lax.axis_index("hp")
    cp = lax.axis_index("cp")
    has_up = hp > 0
    has_down = hp < n_hp - 1
    has_next = cp < n_cp - 1
    has_prev = cp > 0
    odd = lax.rem(cp, 2) == 1

    slab_order = [(k, 1) for k in range(3)] + [(k, di) for di in (0, 2) for k in range(3)]

    def weight_copy(layer, slot, k, di):
        slab = k * 3 + di
        return pltpu.make_async_copy(w_ref.at[layer, slab], wbuf.at[slot, slab], w_sem.at[slot, slab])

    def start_weights(layer, slot):
        for k, di in slab_order:
            weight_copy(layer, slot, k, di).start()

    lat_copies = [pltpu.make_async_copy(lat_ref, raw.at[0, 1, pl.ds(2, frames)], lat_sem.at[0]),
                  pltpu.make_async_copy(lat_ref, xres, lat_sem.at[1])]
    small_copies = [pltpu.make_async_copy(ref, small.at[i], small_sem.at[i]) for i, ref in enumerate((b_ref, g_ref, be_ref))]
    for copy in lat_copies + small_copies:
        copy.start()

    def others(visit):
        @pl.loop(0, n_hp)
        def _(i):
            for j in range(n_cp):
                target = {"hp": lax.rem(hp + n_hp // 2 + i, n_hp), "cp": lax.rem(cp + n_cp // 2 + j, n_cp)}
                if j == n_cp // 2:
                    pl.when(i != n_hp // 2)(functools.partial(visit, target))
                else:
                    visit(target)

    barrier = pltpu.get_barrier_semaphore()
    with jax.named_scope("entry_signals"):
        others(lambda target: pl.semaphore_signal(barrier, inc=1, device_id=target, device_id_type=MESH))

    def row_copy(slot, c, to_down):
        span = pl.ds(2 + c * CHUNK, CHUNK)
        row = 0 if to_down else 2
        return pltpu.make_async_remote_copy(
            src_ref=raw.at[slot, 1, span], dst_ref=raw.at[slot, row, span],
            send_sem=send_sem.at[slot, row, c], recv_sem=recv_sem.at[slot, row, c],
            device_id={"hp": hp + (1 if to_down else -1)}, device_id_type=MESH)

    def time_copy(slot, dh):
        row = dh if dh is None else (0 if dh == 1 else 2)
        row = 1 if dh == 0 else row
        return pltpu.make_async_remote_copy(
            src_ref=raw.at[slot, 1, pl.ds(frames, 2)], dst_ref=raw.at[slot, row, pl.ds(0, 2)],
            send_sem=send_sem.at[slot, row, n_chunks], recv_sem=recv_sem.at[slot, row, n_chunks],
            device_id={"hp": hp + dh, "cp": cp + 1}, device_id_type=MESH)

    def start_rows(slot, c):
        @pl.when(has_up)
        def _():
            row_copy(slot, c, False).start()

        @pl.when(has_down)
        def _():
            row_copy(slot, c, True).start()

    def start_times(slot):
        @pl.when(has_next)
        def _():
            time_copy(slot, 0).start()

        @pl.when(jnp.logical_and(has_next, has_up))
        def _():
            time_copy(slot, -1).start()

        @pl.when(jnp.logical_and(has_next, has_down))
        def _():
            time_copy(slot, 1).start()

    def wait_sends(slot):
        for c in range(n_chunks):
            @pl.when(has_up)
            def _():
                row_copy(slot, c, False).wait_send()

            @pl.when(has_down)
            def _():
                row_copy(slot, c, True).wait_send()

        @pl.when(has_next)
        def _():
            time_copy(slot, 0).wait_send()

        @pl.when(jnp.logical_and(has_next, has_up))
        def _():
            time_copy(slot, -1).wait_send()

        @pl.when(jnp.logical_and(has_next, has_down))
        def _():
            time_copy(slot, 1).wait_send()

    for row, ok in ((0, has_up), (2, has_down)):
        @pl.when(jnp.logical_not(ok))
        def _():
            @pl.loop(0, frames + 2)
            def _(f):
                for slot in range(2):
                    raw[slot, row, f] = jnp.zeros((width, channels), jnp.bfloat16)

    @pl.when(jnp.logical_not(has_prev))
    def _():
        for slot in range(2):
            for row in range(3):
                for f in range(2):
                    raw[slot, row, f] = jnp.zeros((width, channels), jnp.bfloat16)

    with jax.named_scope("lat_wait"):
        for copy in lat_copies:
            copy.wait()
    start_weights(0, 0)

    def fold(v):
        return jnp.sum(v.reshape(-1, 8, v.shape[-1]), axis=0)

    ssum[...] = jnp.zeros_like(ssum)

    @pl.loop(0, frames)
    def _(f):
        v = xres[f].astype(jnp.float32)
        ssum[0] += fold(v)
        ssum[1] += fold(v * v)

    lane = lax.broadcasted_iota(jnp.int32, (8, 128), 1)
    sub = lax.broadcasted_iota(jnp.int32, (8, 128), 0)
    pick = (lane & 15) == sub

    me = hp * n_cp + cp

    def send_sums(layer):
        for s in range(2):
            for i in range(4):
                st8[s * 4 + i : s * 4 + i + 1, :] = jnp.sum(ssum[s, :, i * 128 : (i + 1) * 128], axis=0, keepdims=True)
        mine = jnp.where(pick, lane_sums(st8[...], lane), 0.0)
        msg[layer] = jnp.sum(mine, axis=0, keepdims=True)
        peers[layer, me] = msg[layer]
        others(lambda target: pltpu.make_async_remote_copy(
            src_ref=msg.at[layer], dst_ref=peers.at[layer, me], send_sem=msg_send.at[layer], recv_sem=msg_recv.at[layer],
            device_id=target, device_id_type=MESH).start())

    def statistics(layer):
        rest = peers.at[layer, pl.ds(0, n_hp * n_cp - 1)]
        pltpu.make_async_copy(rest, rest, msg_recv.at[layer]).wait()
        pltpu.make_async_copy(rest, rest, msg_send.at[layer]).wait()
        total = tree_sum([peers[layer, i] for i in range(n_hp * n_cp)])
        st8[...] = lane_sums(jnp.where(pick, jnp.broadcast_to(total, (8, 128)), 0.0), lane)
        mean = st8[0:4, :] * (1.0 / total_count)
        var = st8[4:8, :] * (1.0 / total_count) - mean * mean
        inv = lax.rsqrt(var + EPS)
        st8[0:4, :] = inv
        st8[4:8, :] = mean * inv
        for i in range(4):
            lanes = slice(i * 128, (i + 1) * 128)
            gamma = 0.5 * params[1, layer, :, lanes]
            scale = gamma * st8[i : i + 1, :]
            shift = 0.5 * params[2, layer, :, lanes] - st8[4 + i : 5 + i, :] * gamma
            for row, ok in ((0, has_up), (1, None), (2, has_down)):
                coef[row, 0:1, lanes] = scale if ok is None else jnp.where(ok, scale, 0.0)
                coef[row, 1:2, lanes] = shift if ok is None else jnp.where(ok, shift, 0.0)

    first_frame = jnp.where(has_prev, 0, 2)
    col = lax.broadcasted_iota(jnp.int32, (width, channels), 0)

    def activate(slot, row, f):
        v = raw[slot, row, jnp.maximum(f, first_frame)].astype(jnp.float32)
        u = v * coef[row, 0:1, :] + coef[row, 1:2, :]
        y = u * jnp.tanh(u) + u
        left = jnp.where(col == 0, 0.0, pltpu.roll(y, 1, 0))
        right = jnp.where(col == width - 1, 0.0, pltpu.roll(y, width - 1, 0))
        for dj, v in enumerate((left, y, right)):
            act[row, f, :, dj * channels : (dj + 1) * channels] = v.astype(jnp.bfloat16)

    def halo_wait(slot, c, row):
        ok = has_up if row == 0 else has_down
        if c == 0:
            @pl.when(jnp.logical_and(ok, has_prev))
            def _():
                time_copy(slot, 1 if row == 0 else -1).wait_recv()

        @pl.when(ok)
        def _():
            row_copy(slot, c, row == 0).wait_recv()

    def conv_chunk(slot, c):
        new = range(c * CHUNK + 2 if c else 0, c * CHUNK + 5)
        for row in (0, 2):
            halo_wait(slot, c, row)
        for f in new:
            activate(slot, 1, f)
        side = [functools.partial(activate, slot, row, f) for f in new for row in (0, 2)]
        total = None
        for n, row in enumerate((1, 0, 2)):
            for k in range(3):
                lhs = act[row, c * CHUNK + k : c * CHUNK + k + CHUNK].reshape(CHUNK * width, 3 * channels)
                part = jnp.dot(lhs, wbuf[slot, k * 3 + row], preferred_element_type=jnp.float32)
                total = part if total is None else total + part
                if n == 0:
                    for work in side[len(side) * k // 3 : len(side) * (k + 1) // 3]:
                        work()
        return total.reshape(CHUNK, width, channels)

    def finish(layer, other, c, y):
        second = lax.rem(layer, 2) == 1
        for f in range(c * CHUNK, (c + 1) * CHUNK):
            h = (y[f - c * CHUNK] + params[0, layer]).astype(jnp.bfloat16).astype(jnp.float32)
            x = xres[f].astype(jnp.float32)
            out = (h + jnp.where(second, x, 0.0)).astype(jnp.bfloat16)
            raw[other, 1, 2 + f] = out
            o_ref[f] = out
            out = out.astype(jnp.float32)
            xres[f] = jnp.where(second, out, x).astype(jnp.bfloat16)
            ssum[0] += fold(out)
            ssum[1] += fold(out * out)

    for copy in small_copies:
        copy.wait()
    for i in range(3):
        for layer in range(LAYERS):
            params[i, layer] = small[i, layer : layer + 1, :]
    with jax.named_scope("entry_wait"):
        pl.semaphore_wait(barrier, n_hp * n_cp - 1)
    with jax.named_scope("send_sums"):
        send_sums(0)
    start_times(0)
    for c in range(n_chunks):
        start_rows(0, c)

    def layer_body(layer, _):
        slot = lax.rem(layer, 2)
        other = 1 - slot
        more = layer < LAYERS - 1

        @pl.when(more)
        def _():
            start_weights(layer + 1, other)

        with jax.named_scope("statistics"):
            statistics(layer)

        @pl.when(layer > 0)
        def _():
            start_rows(slot, n_chunks - 1)

        with jax.named_scope("w_wait"):
            @pl.when(has_prev)
            def _():
                time_copy(slot, 0).wait_recv()

            for k, di in slab_order:
                weight_copy(layer, slot, k, di).wait()

        ssum[...] = jnp.zeros_like(ssum)
        for c in range(n_chunks):
            with jax.named_scope(f"chunk{c}"):
                finish(layer, other, c, conv_chunk(slot, c))
            if c < n_chunks - 1:
                @pl.when(more if c < 2 else jnp.logical_and(more, odd))
                def _():
                    start_rows(other, c)

        with jax.named_scope("send_wait"):
            wait_sends(slot)
        @pl.when(more)
        def _():
            with jax.named_scope("send_sums"):
                send_sums(layer + 1)
            with jax.named_scope("send_rest"):
                start_times(other)

                @pl.when(jnp.logical_not(odd))
                def _():
                    start_rows(other, n_chunks - 2)

        return 0

    lax.fori_loop(0, LAYERS, layer_body, 0)


def solution(mesh):
    n_hp, n_cp = mesh.shape["hp"], mesh.shape["cp"]

    def local_decode(lat, conv_w, conv_b, gn_gamma, gn_beta):
        frames, rows, width, channels = lat.shape
        n_chunks = frames // CHUNK
        total_count = float(frames * n_cp * rows * n_hp * width * (channels // GROUPS))
        hbm_spec = pl.BlockSpec(memory_space=pltpu.HBM)
        bf16, f32 = jnp.bfloat16, jnp.float32
        flops = LAYERS * 2 * frames * width * 27 * channels * channels
        out = pl.pallas_call(
            functools.partial(decode_kernel, n_hp, n_cp, total_count),
            out_shape=jax.ShapeDtypeStruct((frames, width, channels), bf16),
            in_specs=[hbm_spec] * 5,
            out_specs=pl.BlockSpec(memory_space=pltpu.VMEM),
            scratch_shapes=[
                pltpu.VMEM((2, 9, 3 * channels, channels), bf16),
                pltpu.VMEM((2, 3, frames + 2, width, channels), bf16),
                pltpu.VMEM((3, frames + 2, width, 3 * channels), bf16),
                pltpu.VMEM((frames, width, channels), bf16),
                pltpu.VMEM((3, LAYERS, channels), f32),
                pltpu.VMEM((3, LAYERS, 1, channels), f32),
                pltpu.VMEM((2, 8, channels), f32),
                pltpu.VMEM((8, 128), f32),
                pltpu.VMEM((3, 8, channels), f32),
                pltpu.VMEM((LAYERS, 1, 128), f32),
                pltpu.VMEM((LAYERS, n_hp * n_cp, 1, 128), f32),
                pltpu.SemaphoreType.DMA((2, 9)),
                pltpu.SemaphoreType.DMA((2,)),
                pltpu.SemaphoreType.DMA((3,)),
                pltpu.SemaphoreType.DMA((2, 3, n_chunks + 1)),
                pltpu.SemaphoreType.DMA((2, 3, n_chunks + 1)),
                pltpu.SemaphoreType.DMA((LAYERS,)),
                pltpu.SemaphoreType.DMA((LAYERS,)),
            ],
            compiler_params=pltpu.CompilerParams(
                collective_id=0, has_side_effects=True, vmem_limit_bytes=46 * 1024 * 1024),
            cost_estimate=pl.CostEstimate(flops=flops, bytes_accessed=conv_w.size * 2, transcendentals=0),
        )(*(pltpu.with_memory_space_constraint(v, pltpu.HBM) for v in (
            lat.reshape(frames, width, channels), conv_w.reshape(LAYERS, 9, 3 * channels, channels),
            conv_b, gn_gamma, gn_beta)))
        return out.reshape(lat.shape)

    video_spec = P(("dp", "cp"), "hp", None, None)
    return jax.shard_map(local_decode, mesh=mesh, in_specs=(video_spec, P(), P(), P(), P()), out_specs=video_spec, check_vma=False)
```

```python
import functools

import jax
import jax.numpy as jnp
from jax import lax
from jax.experimental import pallas as pl
from jax.experimental.pallas import tpu as pltpu
from jax.sharding import PartitionSpec as P

GROUPS = 32
EPS = 1e-6
LAYERS = 4
MESH = pl.DeviceIdType.MESH
CHUNK = 3


def lane_sums(y, lane):
    for s in (1, 4):
        place = (lane // s) & 3
        total = y
        for d in (-3, -2, -1, 1, 2, 3):
            inside = jnp.logical_and(place + d >= 0, place + d <= 3)
            total = total + jnp.where(inside, pltpu.roll(y, (-d * s) % 128, 1), 0.0)
        y = total
    return y


def tree_sum(terms):
    while len(terms) > 1:
        terms = [a + b for a, b in zip(terms[::2], terms[1::2])] + terms[len(terms) & ~1 :]
    return terms[0]


def decode_kernel(n_hp, n_cp, total_count, lat_ref, w_ref, b_ref, g_ref, be_ref, o_ref,
                  wbuf, raw, act, xres, small, params, ssum, st8, coef, msg, peers,
                  w_sem, lat_sem, small_sem, send_sem, recv_sem, msg_send, msg_recv):
    frames, width, channels = xres.shape
    n_chunks = frames // CHUNK
    hp = lax.axis_index("hp")
    cp = lax.axis_index("cp")
    has_up = hp > 0
    has_down = hp < n_hp - 1
    has_next = cp < n_cp - 1
    has_prev = cp > 0
    odd = lax.rem(cp, 2) == 1

    slab_order = [(k, 1) for k in range(3)] + [(k, di) for di in (0, 2) for k in range(3)]

    def weight_copy(layer, slot, k, di):
        slab = k * 3 + di
        return pltpu.make_async_copy(w_ref.at[layer, slab], wbuf.at[slot, slab], w_sem.at[slot, slab])

    def start_weights(layer, slot):
        for k, di in slab_order:
            weight_copy(layer, slot, k, di).start()

    lat_copies = [pltpu.make_async_copy(lat_ref, raw.at[0, 1, pl.ds(2, frames)], lat_sem.at[0]),
                  pltpu.make_async_copy(lat_ref, xres, lat_sem.at[1])]
    small_copies = [pltpu.make_async_copy(ref, small.at[i], small_sem.at[i]) for i, ref in enumerate((b_ref, g_ref, be_ref))]
    for copy in lat_copies + small_copies:
        copy.start()

    def others(visit):
        @pl.loop(0, n_hp)
        def _(i):
            for j in range(n_cp):
                target = {"hp": lax.rem(hp + n_hp // 2 + i, n_hp), "cp": lax.rem(cp + n_cp // 2 + j, n_cp)}
                if j == n_cp // 2:
                    pl.when(i != n_hp // 2)(functools.partial(visit, target))
                else:
                    visit(target)

    barrier = pltpu.get_barrier_semaphore()
    with jax.named_scope("entry_signals"):
        others(lambda target: pl.semaphore_signal(barrier, inc=1, device_id=target, device_id_type=MESH))

    def row_copy(slot, c, to_down):
        span = pl.ds(2 + c * CHUNK, CHUNK)
        row = 0 if to_down else 2
        return pltpu.make_async_remote_copy(
            src_ref=raw.at[slot, 1, span], dst_ref=raw.at[slot, row, span],
            send_sem=send_sem.at[slot, row, c], recv_sem=recv_sem.at[slot, row, c],
            device_id={"hp": hp + (1 if to_down else -1)}, device_id_type=MESH)

    def time_copy(slot, dh):
        row = dh if dh is None else (0 if dh == 1 else 2)
        row = 1 if dh == 0 else row
        return pltpu.make_async_remote_copy(
            src_ref=raw.at[slot, 1, pl.ds(frames, 2)], dst_ref=raw.at[slot, row, pl.ds(0, 2)],
            send_sem=send_sem.at[slot, row, n_chunks], recv_sem=recv_sem.at[slot, row, n_chunks],
            device_id={"hp": hp + dh, "cp": cp + 1}, device_id_type=MESH)

    def start_rows(slot, c):
        @pl.when(has_up)
        def _():
            row_copy(slot, c, False).start()

        @pl.when(has_down)
        def _():
            row_copy(slot, c, True).start()

    def start_times(slot):
        @pl.when(has_next)
        def _():
            time_copy(slot, 0).start()

        @pl.when(jnp.logical_and(has_next, has_up))
        def _():
            time_copy(slot, -1).start()

        @pl.when(jnp.logical_and(has_next, has_down))
        def _():
            time_copy(slot, 1).start()

    def wait_sends(slot):
        for c in range(n_chunks):
            @pl.when(has_up)
            def _():
                row_copy(slot, c, False).wait_send()

            @pl.when(has_down)
            def _():
                row_copy(slot, c, True).wait_send()

        @pl.when(has_next)
        def _():
            time_copy(slot, 0).wait_send()

        @pl.when(jnp.logical_and(has_next, has_up))
        def _():
            time_copy(slot, -1).wait_send()

        @pl.when(jnp.logical_and(has_next, has_down))
        def _():
            time_copy(slot, 1).wait_send()

    for row, ok in ((0, has_up), (2, has_down)):
        @pl.when(jnp.logical_not(ok))
        def _():
            @pl.loop(0, frames + 2)
            def _(f):
                for slot in range(2):
                    raw[slot, row, f] = jnp.zeros((width, channels), jnp.bfloat16)

    @pl.when(jnp.logical_not(has_prev))
    def _():
        for slot in range(2):
            for row in range(3):
                for f in range(2):
                    raw[slot, row, f] = jnp.zeros((width, channels), jnp.bfloat16)

    with jax.named_scope("lat_wait"):
        for copy in lat_copies:
            copy.wait()
    start_weights(0, 0)

    def fold(v):
        return jnp.sum(v.reshape(-1, 8, v.shape[-1]), axis=0)

    ssum[...] = jnp.zeros_like(ssum)

    @pl.loop(0, frames)
    def _(f):
        v = xres[f].astype(jnp.float32)
        ssum[0] += fold(v)
        ssum[1] += fold(v * v)

    lane = lax.broadcasted_iota(jnp.int32, (8, 128), 1)
    sub = lax.broadcasted_iota(jnp.int32, (8, 128), 0)
    pick = (lane & 15) == sub

    me = hp * n_cp + cp

    def send_sums(layer):
        for s in range(2):
            for i in range(4):
                st8[s * 4 + i : s * 4 + i + 1, :] = jnp.sum(ssum[s, :, i * 128 : (i + 1) * 128], axis=0, keepdims=True)
        mine = jnp.where(pick, lane_sums(st8[...], lane), 0.0)
        msg[layer] = jnp.sum(mine, axis=0, keepdims=True)
        peers[layer, me] = msg[layer]
        others(lambda target: pltpu.make_async_remote_copy(
            src_ref=msg.at[layer], dst_ref=peers.at[layer, me], send_sem=msg_send.at[layer], recv_sem=msg_recv.at[layer],
            device_id=target, device_id_type=MESH).start())

    def statistics(layer):
        rest = peers.at[layer, pl.ds(0, n_hp * n_cp - 1)]
        pltpu.make_async_copy(rest, rest, msg_recv.at[layer]).wait()
        pltpu.make_async_copy(rest, rest, msg_send.at[layer]).wait()
        total = tree_sum([peers[layer, i] for i in range(n_hp * n_cp)])
        st8[...] = lane_sums(jnp.where(pick, jnp.broadcast_to(total, (8, 128)), 0.0), lane)
        mean = st8[0:4, :] * (1.0 / total_count)
        var = st8[4:8, :] * (1.0 / total_count) - mean * mean
        inv = lax.rsqrt(var + EPS)
        st8[0:4, :] = inv
        st8[4:8, :] = mean * inv
        for i in range(4):
            lanes = slice(i * 128, (i + 1) * 128)
            gamma = 0.5 * params[1, layer, :, lanes]
            scale = gamma * st8[i : i + 1, :]
            shift = 0.5 * params[2, layer, :, lanes] - st8[4 + i : 5 + i, :] * gamma
            for row, ok in ((0, has_up), (1, None), (2, has_down)):
                coef[row, 0:1, lanes] = scale if ok is None else jnp.where(ok, scale, 0.0)
                coef[row, 1:2, lanes] = shift if ok is None else jnp.where(ok, shift, 0.0)

    first_frame = jnp.where(has_prev, 0, 2)
    col = lax.broadcasted_iota(jnp.int32, (width, channels), 0)

    def activate(slot, row, f):
        v = raw[slot, row, jnp.maximum(f, first_frame)].astype(jnp.float32)
        u = v * coef[row, 0:1, :] + coef[row, 1:2, :]
        y = u * jnp.tanh(u) + u
        left = jnp.where(col == 0, 0.0, pltpu.roll(y, 1, 0))
        right = jnp.where(col == width - 1, 0.0, pltpu.roll(y, width - 1, 0))
        for dj, v in enumerate((left, y, right)):
            act[row, f, :, dj * channels : (dj + 1) * channels] = v.astype(jnp.bfloat16)

    def halo_wait(slot, c, row):
        ok = has_up if row == 0 else has_down
        if c == 0:
            @pl.when(jnp.logical_and(ok, has_prev))
            def _():
                time_copy(slot, 1 if row == 0 else -1).wait_recv()

        @pl.when(ok)
        def _():
            row_copy(slot, c, row == 0).wait_recv()

    def conv_chunk(slot, c):
        new = range(c * CHUNK + 2 if c else 0, c * CHUNK + 5)
        for row in (0, 2):
            halo_wait(slot, c, row)
        for f in new:
            activate(slot, 1, f)
        side = [functools.partial(activate, slot, row, f) for f in new for row in (0, 2)]
        total = None
        for n, row in enumerate((1, 0, 2)):
            for k in range(3):
                lhs = act[row, c * CHUNK + k : c * CHUNK + k + CHUNK].reshape(CHUNK * width, 3 * channels)
                part = jnp.dot(lhs, wbuf[slot, k * 3 + row], preferred_element_type=jnp.float32)
                total = part if total is None else total + part
                if n == 0:
                    for work in side[len(side) * k // 3 : len(side) * (k + 1) // 3]:
                        work()
        return total.reshape(CHUNK, width, channels)

    def finish(layer, other, c, y):
        second = lax.rem(layer, 2) == 1
        for f in range(c * CHUNK, (c + 1) * CHUNK):
            h = (y[f - c * CHUNK] + params[0, layer]).astype(jnp.bfloat16).astype(jnp.float32)
            x = xres[f].astype(jnp.float32)
            out = (h + jnp.where(second, x, 0.0)).astype(jnp.bfloat16)
            raw[other, 1, 2 + f] = out
            o_ref[f] = out
            out = out.astype(jnp.float32)
            xres[f] = jnp.where(second, out, x).astype(jnp.bfloat16)
            ssum[0] += fold(out)
            ssum[1] += fold(out * out)

    for copy in small_copies:
        copy.wait()
    for i in range(3):
        for layer in range(LAYERS):
            params[i, layer] = small[i, layer : layer + 1, :]
    with jax.named_scope("entry_wait"):
        pl.semaphore_wait(barrier, n_hp * n_cp - 1)
    with jax.named_scope("send_sums"):
        send_sums(0)
    start_times(0)
    for c in range(n_chunks):
        start_rows(0, c)

    def layer_body(layer, _):
        slot = lax.rem(layer, 2)
        other = 1 - slot
        more = layer < LAYERS - 1

        @pl.when(more)
        def _():
            start_weights(layer + 1, other)

        with jax.named_scope("statistics"):
            statistics(layer)

        @pl.when(jnp.logical_and(layer > 0, jnp.logical_not(odd)))
        def _():
            for c in range(2, n_chunks):
                start_rows(slot, c)

        with jax.named_scope("w_wait"):
            @pl.when(has_prev)
            def _():
                time_copy(slot, 0).wait_recv()

            for k, di in slab_order:
                weight_copy(layer, slot, k, di).wait()

        ssum[...] = jnp.zeros_like(ssum)
        for c in range(n_chunks):
            with jax.named_scope(f"chunk{c}"):
                finish(layer, other, c, conv_chunk(slot, c))
            if c < n_chunks - 1:
                @pl.when(more if c < 2 else jnp.logical_and(more, odd))
                def _():
                    start_rows(other, c)
            if c == 0:
                @pl.when(jnp.logical_and(layer > 0, odd))
                def _():
                    start_rows(slot, n_chunks - 1)

        with jax.named_scope("send_wait"):
            wait_sends(slot)
        @pl.when(more)
        def _():
            with jax.named_scope("send_sums"):
                send_sums(layer + 1)
            with jax.named_scope("send_rest"):
                start_times(other)

        return 0

    lax.fori_loop(0, LAYERS, layer_body, 0)


def solution(mesh):
    n_hp, n_cp = mesh.shape["hp"], mesh.shape["cp"]

    def local_decode(lat, conv_w, conv_b, gn_gamma, gn_beta):
        frames, rows, width, channels = lat.shape
        n_chunks = frames // CHUNK
        total_count = float(frames * n_cp * rows * n_hp * width * (channels // GROUPS))
        hbm_spec = pl.BlockSpec(memory_space=pltpu.HBM)
        bf16, f32 = jnp.bfloat16, jnp.float32
        flops = LAYERS * 2 * frames * width * 27 * channels * channels
        out = pl.pallas_call(
            functools.partial(decode_kernel, n_hp, n_cp, total_count),
            out_shape=jax.ShapeDtypeStruct((frames, width, channels), bf16),
            in_specs=[hbm_spec] * 5,
            out_specs=pl.BlockSpec(memory_space=pltpu.VMEM),
            scratch_shapes=[
                pltpu.VMEM((2, 9, 3 * channels, channels), bf16),
                pltpu.VMEM((2, 3, frames + 2, width, channels), bf16),
                pltpu.VMEM((3, frames + 2, width, 3 * channels), bf16),
                pltpu.VMEM((frames, width, channels), bf16),
                pltpu.VMEM((3, LAYERS, channels), f32),
                pltpu.VMEM((3, LAYERS, 1, channels), f32),
                pltpu.VMEM((2, 8, channels), f32),
                pltpu.VMEM((8, 128), f32),
                pltpu.VMEM((3, 8, channels), f32),
                pltpu.VMEM((LAYERS, 1, 128), f32),
                pltpu.VMEM((LAYERS, n_hp * n_cp, 1, 128), f32),
                pltpu.SemaphoreType.DMA((2, 9)),
                pltpu.SemaphoreType.DMA((2,)),
                pltpu.SemaphoreType.DMA((3,)),
                pltpu.SemaphoreType.DMA((2, 3, n_chunks + 1)),
                pltpu.SemaphoreType.DMA((2, 3, n_chunks + 1)),
                pltpu.SemaphoreType.DMA((LAYERS,)),
                pltpu.SemaphoreType.DMA((LAYERS,)),
            ],
            compiler_params=pltpu.CompilerParams(
                collective_id=0, has_side_effects=True, vmem_limit_bytes=46 * 1024 * 1024),
            cost_estimate=pl.CostEstimate(flops=flops, bytes_accessed=conv_w.size * 2, transcendentals=0),
        )(*(pltpu.with_memory_space_constraint(v, pltpu.HBM) for v in (
            lat.reshape(frames, width, channels), conv_w.reshape(LAYERS, 9, 3 * channels, channels),
            conv_b, gn_gamma, gn_beta)))
        return out.reshape(lat.shape)

    video_spec = P(("dp", "cp"), "hp", None, None)
    return jax.shard_map(local_decode, mesh=mesh, in_specs=(video_spec, P(), P(), P(), P()), out_specs=video_spec, check_vma=False)
```

```python
import functools

import jax
import jax.numpy as jnp
from jax import lax
from jax.experimental import pallas as pl
from jax.experimental.pallas import tpu as pltpu
from jax.sharding import PartitionSpec as P

GROUPS = 32
EPS = 1e-6
LAYERS = 4
MESH = pl.DeviceIdType.MESH
CHUNK = 3


def lane_sums(y, lane):
    for s in (1, 4):
        place = (lane // s) & 3
        total = y
        for d in (-3, -2, -1, 1, 2, 3):
            inside = jnp.logical_and(place + d >= 0, place + d <= 3)
            total = total + jnp.where(inside, pltpu.roll(y, (-d * s) % 128, 1), 0.0)
        y = total
    return y


def tree_sum(terms):
    while len(terms) > 1:
        terms = [a + b for a, b in zip(terms[::2], terms[1::2])] + terms[len(terms) & ~1 :]
    return terms[0]


def decode_kernel(n_hp, n_cp, total_count, lat_ref, w_ref, b_ref, g_ref, be_ref, o_ref,
                  wbuf, raw, act, xres, small, params, ssum, st8, coef, msg, peers,
                  w_sem, lat_sem, small_sem, send_sem, recv_sem, msg_send, msg_recv):
    frames, width, channels = xres.shape
    n_chunks = frames // CHUNK
    hp = lax.axis_index("hp")
    cp = lax.axis_index("cp")
    has_up = hp > 0
    has_down = hp < n_hp - 1
    has_next = cp < n_cp - 1
    has_prev = cp > 0
    odd = lax.rem(cp, 2) == 1

    slab_order = [(k, 1) for k in range(3)] + [(k, di) for di in (0, 2) for k in range(3)]

    def weight_copy(layer, slot, k, di):
        slab = k * 3 + di
        return pltpu.make_async_copy(w_ref.at[layer, slab], wbuf.at[slot, slab], w_sem.at[slot, slab])

    def start_weights(layer, slot):
        for k, di in slab_order:
            weight_copy(layer, slot, k, di).start()

    lat_copies = [pltpu.make_async_copy(lat_ref, raw.at[0, 1, pl.ds(2, frames)], lat_sem.at[0]),
                  pltpu.make_async_copy(lat_ref, xres, lat_sem.at[1])]
    small_copies = [pltpu.make_async_copy(ref, small.at[i], small_sem.at[i]) for i, ref in enumerate((b_ref, g_ref, be_ref))]
    for copy in lat_copies + small_copies:
        copy.start()

    def others(visit):
        @pl.loop(0, n_hp)
        def _(i):
            for j in range(n_cp):
                target = {"hp": lax.rem(hp + n_hp // 2 + i, n_hp), "cp": lax.rem(cp + n_cp // 2 + j, n_cp)}
                if j == n_cp // 2:
                    pl.when(i != n_hp // 2)(functools.partial(visit, target))
                else:
                    visit(target)

    barrier = pltpu.get_barrier_semaphore()
    with jax.named_scope("entry_signals"):
        others(lambda target: pl.semaphore_signal(barrier, inc=1, device_id=target, device_id_type=MESH))

    def row_copy(slot, c, to_down):
        span = pl.ds(2 + c * CHUNK, CHUNK)
        row = 0 if to_down else 2
        return pltpu.make_async_remote_copy(
            src_ref=raw.at[slot, 1, span], dst_ref=raw.at[slot, row, span],
            send_sem=send_sem.at[slot, row, c], recv_sem=recv_sem.at[slot, row, c],
            device_id={"hp": hp + (1 if to_down else -1)}, device_id_type=MESH)

    def time_copy(slot, dh):
        row = dh if dh is None else (0 if dh == 1 else 2)
        row = 1 if dh == 0 else row
        return pltpu.make_async_remote_copy(
            src_ref=raw.at[slot, 1, pl.ds(frames, 2)], dst_ref=raw.at[slot, row, pl.ds(0, 2)],
            send_sem=send_sem.at[slot, row, n_chunks], recv_sem=recv_sem.at[slot, row, n_chunks],
            device_id={"hp": hp + dh, "cp": cp + 1}, device_id_type=MESH)

    def start_rows(slot, c):
        @pl.when(has_up)
        def _():
            row_copy(slot, c, False).start()

        @pl.when(has_down)
        def _():
            row_copy(slot, c, True).start()

    def start_times(slot):
        @pl.when(has_next)
        def _():
            time_copy(slot, 0).start()

        @pl.when(jnp.logical_and(has_next, has_up))
        def _():
            time_copy(slot, -1).start()

        @pl.when(jnp.logical_and(has_next, has_down))
        def _():
            time_copy(slot, 1).start()

    def wait_sends(slot):
        for c in range(n_chunks):
            @pl.when(has_up)
            def _():
                row_copy(slot, c, False).wait_send()

            @pl.when(has_down)
            def _():
                row_copy(slot, c, True).wait_send()

        @pl.when(has_next)
        def _():
            time_copy(slot, 0).wait_send()

        @pl.when(jnp.logical_and(has_next, has_up))
        def _():
            time_copy(slot, -1).wait_send()

        @pl.when(jnp.logical_and(has_next, has_down))
        def _():
            time_copy(slot, 1).wait_send()

    for row, ok in ((0, has_up), (2, has_down)):
        @pl.when(jnp.logical_not(ok))
        def _():
            @pl.loop(0, frames + 2)
            def _(f):
                for slot in range(2):
                    raw[slot, row, f] = jnp.zeros((width, channels), jnp.bfloat16)

    @pl.when(jnp.logical_not(has_prev))
    def _():
        for slot in range(2):
            for row in range(3):
                for f in range(2):
                    raw[slot, row, f] = jnp.zeros((width, channels), jnp.bfloat16)

    with jax.named_scope("lat_wait"):
        for copy in lat_copies:
            copy.wait()
    start_weights(0, 0)

    def fold(v):
        return jnp.sum(v.reshape(-1, 8, v.shape[-1]), axis=0)

    ssum[...] = jnp.zeros_like(ssum)

    @pl.loop(0, frames)
    def _(f):
        v = xres[f].astype(jnp.float32)
        ssum[0] += fold(v)
        ssum[1] += fold(v * v)

    lane = lax.broadcasted_iota(jnp.int32, (8, 128), 1)
    sub = lax.broadcasted_iota(jnp.int32, (8, 128), 0)
    pick = (lane & 15) == sub

    me = hp * n_cp + cp

    def send_sums(layer):
        for s in range(2):
            for i in range(4):
                st8[s * 4 + i : s * 4 + i + 1, :] = jnp.sum(ssum[s, :, i * 128 : (i + 1) * 128], axis=0, keepdims=True)
        mine = jnp.where(pick, lane_sums(st8[...], lane), 0.0)
        msg[layer] = jnp.sum(mine, axis=0, keepdims=True)
        peers[layer, me] = msg[layer]
        others(lambda target: pltpu.make_async_remote_copy(
            src_ref=msg.at[layer], dst_ref=peers.at[layer, me], send_sem=msg_send.at[layer], recv_sem=msg_recv.at[layer],
            device_id=target, device_id_type=MESH).start())

    def statistics(layer):
        rest = peers.at[layer, pl.ds(0, n_hp * n_cp - 1)]
        pltpu.make_async_copy(rest, rest, msg_recv.at[layer]).wait()
        pltpu.make_async_copy(rest, rest, msg_send.at[layer]).wait()
        total = tree_sum([peers[layer, i] for i in range(n_hp * n_cp)])
        st8[...] = lane_sums(jnp.where(pick, jnp.broadcast_to(total, (8, 128)), 0.0), lane)
        mean = st8[0:4, :] * (1.0 / total_count)
        var = st8[4:8, :] * (1.0 / total_count) - mean * mean
        inv = lax.rsqrt(var + EPS)
        st8[0:4, :] = inv
        st8[4:8, :] = mean * inv
        for i in range(4):
            lanes = slice(i * 128, (i + 1) * 128)
            gamma = 0.5 * params[1, layer, :, lanes]
            scale = gamma * st8[i : i + 1, :]
            shift = 0.5 * params[2, layer, :, lanes] - st8[4 + i : 5 + i, :] * gamma
            for row, ok in ((0, has_up), (1, None), (2, has_down)):
                coef[row, 0:1, lanes] = scale if ok is None else jnp.where(ok, scale, 0.0)
                coef[row, 1:2, lanes] = shift if ok is None else jnp.where(ok, shift, 0.0)

    first_frame = jnp.where(has_prev, 0, 2)
    col = lax.broadcasted_iota(jnp.int32, (width, channels), 0)

    def activate(slot, row, f):
        v = raw[slot, row, jnp.maximum(f, first_frame)].astype(jnp.float32)
        u = v * coef[row, 0:1, :] + coef[row, 1:2, :]
        y = u * jnp.tanh(u) + u
        left = jnp.where(col == 0, 0.0, pltpu.roll(y, 1, 0))
        right = jnp.where(col == width - 1, 0.0, pltpu.roll(y, width - 1, 0))
        for dj, v in enumerate((left, y, right)):
            act[row, f, :, dj * channels : (dj + 1) * channels] = v.astype(jnp.bfloat16)

    def halo_wait(slot, c, row):
        ok = has_up if row == 0 else has_down
        if c == 0:
            @pl.when(jnp.logical_and(ok, has_prev))
            def _():
                time_copy(slot, 1 if row == 0 else -1).wait_recv()

        @pl.when(ok)
        def _():
            row_copy(slot, c, row == 0).wait_recv()

    def conv_chunk(slot, c):
        new = range(c * CHUNK + 2 if c else 0, c * CHUNK + 5)
        for row in (0, 2):
            halo_wait(slot, c, row)
        for f in new:
            activate(slot, 1, f)
        side = [functools.partial(activate, slot, row, f) for f in new for row in (0, 2)]
        total = None
        for n, row in enumerate((1, 0, 2)):
            for k in range(3):
                lhs = act[row, c * CHUNK + k : c * CHUNK + k + CHUNK].reshape(CHUNK * width, 3 * channels)
                part = jnp.dot(lhs, wbuf[slot, k * 3 + row], preferred_element_type=jnp.float32)
                total = part if total is None else total + part
                if n == 0:
                    for work in side[len(side) * k // 3 : len(side) * (k + 1) // 3]:
                        work()
        return total.reshape(CHUNK, width, channels)

    def finish(layer, other, c, y):
        second = lax.rem(layer, 2) == 1
        for f in range(c * CHUNK, (c + 1) * CHUNK):
            h = (y[f - c * CHUNK] + params[0, layer]).astype(jnp.bfloat16).astype(jnp.float32)
            x = xres[f].astype(jnp.float32)
            out = (h + jnp.where(second, x, 0.0)).astype(jnp.bfloat16)
            raw[other, 1, 2 + f] = out
            o_ref[f] = out
            out = out.astype(jnp.float32)
            xres[f] = jnp.where(second, out, x).astype(jnp.bfloat16)
            ssum[0] += fold(out)
            ssum[1] += fold(out * out)

    for copy in small_copies:
        copy.wait()
    for i in range(3):
        for layer in range(LAYERS):
            params[i, layer] = small[i, layer : layer + 1, :]
    with jax.named_scope("entry_wait"):
        pl.semaphore_wait(barrier, n_hp * n_cp - 1)
    with jax.named_scope("send_sums"):
        send_sums(0)
    start_times(0)
    for c in range(n_chunks):
        start_rows(0, c)

    def layer_body(layer, _):
        slot = lax.rem(layer, 2)
        other = 1 - slot
        more = layer < LAYERS - 1

        @pl.when(more)
        def _():
            start_weights(layer + 1, other)

        with jax.named_scope("statistics"):
            statistics(layer)

        with jax.named_scope("w_wait"):
            @pl.when(has_prev)
            def _():
                time_copy(slot, 0).wait_recv()

            for k, di in slab_order:
                weight_copy(layer, slot, k, di).wait()

        ssum[...] = jnp.zeros_like(ssum)
        for c in range(n_chunks):
            with jax.named_scope(f"chunk{c}"):
                finish(layer, other, c, conv_chunk(slot, c))
            if c < n_chunks - 1:
                @pl.when(more if c < 2 else jnp.logical_and(more, odd))
                def _():
                    start_rows(other, c)

        with jax.named_scope("send_wait"):
            wait_sends(slot)
        @pl.when(more)
        def _():
            with jax.named_scope("send_sums"):
                send_sums(layer + 1)
            with jax.named_scope("send_rest"):
                start_times(other)

                @pl.when(jnp.logical_not(odd))
                def _():
                    start_rows(other, n_chunks - 2)

                start_rows(other, n_chunks - 1)

        return 0

    lax.fori_loop(0, LAYERS, layer_body, 0)


def solution(mesh):
    n_hp, n_cp = mesh.shape["hp"], mesh.shape["cp"]

    def local_decode(lat, conv_w, conv_b, gn_gamma, gn_beta):
        frames, rows, width, channels = lat.shape
        n_chunks = frames // CHUNK
        total_count = float(frames * n_cp * rows * n_hp * width * (channels // GROUPS))
        hbm_spec = pl.BlockSpec(memory_space=pltpu.HBM)
        bf16, f32 = jnp.bfloat16, jnp.float32
        flops = LAYERS * 2 * frames * width * 27 * channels * channels
        out = pl.pallas_call(
            functools.partial(decode_kernel, n_hp, n_cp, total_count),
            out_shape=jax.ShapeDtypeStruct((frames, width, channels), bf16),
            in_specs=[hbm_spec] * 5,
            out_specs=pl.BlockSpec(memory_space=pltpu.VMEM),
            scratch_shapes=[
                pltpu.VMEM((2, 9, 3 * channels, channels), bf16),
                pltpu.VMEM((2, 3, frames + 2, width, channels), bf16),
                pltpu.VMEM((3, frames + 2, width, 3 * channels), bf16),
                pltpu.VMEM((frames, width, channels), bf16),
                pltpu.VMEM((3, LAYERS, channels), f32),
                pltpu.VMEM((3, LAYERS, 1, channels), f32),
                pltpu.VMEM((2, 8, channels), f32),
                pltpu.VMEM((8, 128), f32),
                pltpu.VMEM((3, 8, channels), f32),
                pltpu.VMEM((LAYERS, 1, 128), f32),
                pltpu.VMEM((LAYERS, n_hp * n_cp, 1, 128), f32),
                pltpu.SemaphoreType.DMA((2, 9)),
                pltpu.SemaphoreType.DMA((2,)),
                pltpu.SemaphoreType.DMA((3,)),
                pltpu.SemaphoreType.DMA((2, 3, n_chunks + 1)),
                pltpu.SemaphoreType.DMA((2, 3, n_chunks + 1)),
                pltpu.SemaphoreType.DMA((LAYERS,)),
                pltpu.SemaphoreType.DMA((LAYERS,)),
            ],
            compiler_params=pltpu.CompilerParams(
                collective_id=0, has_side_effects=True, vmem_limit_bytes=46 * 1024 * 1024),
            cost_estimate=pl.CostEstimate(flops=flops, bytes_accessed=conv_w.size * 2, transcendentals=0),
        )(*(pltpu.with_memory_space_constraint(v, pltpu.HBM) for v in (
            lat.reshape(frames, width, channels), conv_w.reshape(LAYERS, 9, 3 * channels, channels),
            conv_b, gn_gamma, gn_beta)))
        return out.reshape(lat.shape)

    video_spec = P(("dp", "cp"), "hp", None, None)
    return jax.shard_map(local_decode, mesh=mesh, in_specs=(video_spec, P(), P(), P(), P()), out_specs=video_spec, check_vma=False)
```

```python
import functools

import jax
import jax.numpy as jnp
from jax import lax
from jax.experimental import pallas as pl
from jax.experimental.pallas import tpu as pltpu
from jax.sharding import PartitionSpec as P

GROUPS = 32
EPS = 1e-6
LAYERS = 4
MESH = pl.DeviceIdType.MESH
CHUNK = 3


def lane_sums(y, lane):
    for s in (1, 4):
        place = (lane // s) & 3
        total = y
        for d in (-3, -2, -1, 1, 2, 3):
            inside = jnp.logical_and(place + d >= 0, place + d <= 3)
            total = total + jnp.where(inside, pltpu.roll(y, (-d * s) % 128, 1), 0.0)
        y = total
    return y


def tree_sum(terms):
    while len(terms) > 1:
        terms = [a + b for a, b in zip(terms[::2], terms[1::2])] + terms[len(terms) & ~1 :]
    return terms[0]


def decode_kernel(n_hp, n_cp, total_count, lat_ref, w_ref, b_ref, g_ref, be_ref, o_ref,
                  wbuf, raw, act, xres, small, params, ssum, st8, coef, msg, peers,
                  w_sem, lat_sem, small_sem, send_sem, recv_sem, msg_send, msg_recv):
    frames, width, channels = xres.shape
    n_chunks = frames // CHUNK
    hp = lax.axis_index("hp")
    cp = lax.axis_index("cp")
    has_up = hp > 0
    has_down = hp < n_hp - 1
    has_next = cp < n_cp - 1
    has_prev = cp > 0

    slab_order = [(k, 1) for k in range(3)] + [(k, di) for di in (0, 2) for k in range(3)]

    def weight_copy(layer, slot, k, di):
        slab = k * 3 + di
        return pltpu.make_async_copy(w_ref.at[layer, slab], wbuf.at[slot, slab], w_sem.at[slot, slab])

    def start_weights(layer, slot):
        for k, di in slab_order:
            weight_copy(layer, slot, k, di).start()

    lat_copies = [pltpu.make_async_copy(lat_ref, raw.at[0, 1, pl.ds(2, frames)], lat_sem.at[0]),
                  pltpu.make_async_copy(lat_ref, xres, lat_sem.at[1])]
    small_copies = [pltpu.make_async_copy(ref, small.at[i], small_sem.at[i]) for i, ref in enumerate((b_ref, g_ref, be_ref))]
    for copy in lat_copies + small_copies:
        copy.start()

    def others(visit):
        @pl.loop(0, n_hp)
        def _(i):
            for j in range(n_cp):
                target = {"hp": lax.rem(hp + n_hp // 2 + i, n_hp), "cp": lax.rem(cp + n_cp // 2 + j, n_cp)}
                if j == n_cp // 2:
                    pl.when(i != n_hp // 2)(functools.partial(visit, target))
                else:
                    visit(target)

    barrier = pltpu.get_barrier_semaphore()
    with jax.named_scope("entry_signals"):
        others(lambda target: pl.semaphore_signal(barrier, inc=1, device_id=target, device_id_type=MESH))

    def row_copy(slot, c, to_down):
        span = pl.ds(2 + c * CHUNK, CHUNK)
        row = 0 if to_down else 2
        return pltpu.make_async_remote_copy(
            src_ref=raw.at[slot, 1, span], dst_ref=raw.at[slot, row, span],
            send_sem=send_sem.at[slot, row, c], recv_sem=recv_sem.at[slot, row, c],
            device_id={"hp": hp + (1 if to_down else -1)}, device_id_type=MESH)

    def time_copy(slot, dh):
        row = dh if dh is None else (0 if dh == 1 else 2)
        row = 1 if dh == 0 else row
        return pltpu.make_async_remote_copy(
            src_ref=raw.at[slot, 1, pl.ds(frames, 2)], dst_ref=raw.at[slot, row, pl.ds(0, 2)],
            send_sem=send_sem.at[slot, row, n_chunks], recv_sem=recv_sem.at[slot, row, n_chunks],
            device_id={"hp": hp + dh, "cp": cp + 1}, device_id_type=MESH)

    def start_rows(slot, c):
        @pl.when(has_up)
        def _():
            row_copy(slot, c, False).start()

        @pl.when(has_down)
        def _():
            row_copy(slot, c, True).start()

    def start_times(slot):
        @pl.when(has_next)
        def _():
            time_copy(slot, 0).start()

        @pl.when(jnp.logical_and(has_next, has_up))
        def _():
            time_copy(slot, -1).start()

        @pl.when(jnp.logical_and(has_next, has_down))
        def _():
            time_copy(slot, 1).start()

    def wait_sends(slot):
        for c in range(n_chunks):
            @pl.when(has_up)
            def _():
                row_copy(slot, c, False).wait_send()

            @pl.when(has_down)
            def _():
                row_copy(slot, c, True).wait_send()

        @pl.when(has_next)
        def _():
            time_copy(slot, 0).wait_send()

        @pl.when(jnp.logical_and(has_next, has_up))
        def _():
            time_copy(slot, -1).wait_send()

        @pl.when(jnp.logical_and(has_next, has_down))
        def _():
            time_copy(slot, 1).wait_send()

    for row, ok in ((0, has_up), (2, has_down)):
        @pl.when(jnp.logical_not(ok))
        def _():
            @pl.loop(0, frames + 2)
            def _(f):
                for slot in range(2):
                    raw[slot, row, f] = jnp.zeros((width, channels), jnp.bfloat16)

    @pl.when(jnp.logical_not(has_prev))
    def _():
        for slot in range(2):
            for row in range(3):
                for f in range(2):
                    raw[slot, row, f] = jnp.zeros((width, channels), jnp.bfloat16)

    with jax.named_scope("lat_wait"):
        for copy in lat_copies:
            copy.wait()
    start_weights(0, 0)

    def fold(v):
        return jnp.sum(v.reshape(-1, 8, v.shape[-1]), axis=0)

    ssum[...] = jnp.zeros_like(ssum)

    @pl.loop(0, frames)
    def _(f):
        v = xres[f].astype(jnp.float32)
        ssum[0] += fold(v)
        ssum[1] += fold(v * v)

    lane = lax.broadcasted_iota(jnp.int32, (8, 128), 1)
    sub = lax.broadcasted_iota(jnp.int32, (8, 128), 0)
    pick = (lane & 15) == sub

    me = hp * n_cp + cp

    def send_sums(layer):
        for s in range(2):
            for i in range(4):
                st8[s * 4 + i : s * 4 + i + 1, :] = jnp.sum(ssum[s, :, i * 128 : (i + 1) * 128], axis=0, keepdims=True)
        mine = jnp.where(pick, lane_sums(st8[...], lane), 0.0)
        msg[layer] = jnp.sum(mine, axis=0, keepdims=True)
        peers[layer, me] = msg[layer]
        others(lambda target: pltpu.make_async_remote_copy(
            src_ref=msg.at[layer], dst_ref=peers.at[layer, me], send_sem=msg_send.at[layer], recv_sem=msg_recv.at[layer],
            device_id=target, device_id_type=MESH).start())

    def statistics(layer):
        rest = peers.at[layer, pl.ds(0, n_hp * n_cp - 1)]
        pltpu.make_async_copy(rest, rest, msg_recv.at[layer]).wait()
        pltpu.make_async_copy(rest, rest, msg_send.at[layer]).wait()
        total = tree_sum([peers[layer, i] for i in range(n_hp * n_cp)])
        st8[...] = lane_sums(jnp.where(pick, jnp.broadcast_to(total, (8, 128)), 0.0), lane)
        mean = st8[0:4, :] * (1.0 / total_count)
        var = st8[4:8, :] * (1.0 / total_count) - mean * mean
        inv = lax.rsqrt(var + EPS)
        st8[0:4, :] = inv
        st8[4:8, :] = mean * inv
        for i in range(4):
            lanes = slice(i * 128, (i + 1) * 128)
            gamma = 0.5 * params[1, layer, :, lanes]
            scale = gamma * st8[i : i + 1, :]
            shift = 0.5 * params[2, layer, :, lanes] - st8[4 + i : 5 + i, :] * gamma
            for row, ok in ((0, has_up), (1, None), (2, has_down)):
                coef[row, 0:1, lanes] = scale if ok is None else jnp.where(ok, scale, 0.0)
                coef[row, 1:2, lanes] = shift if ok is None else jnp.where(ok, shift, 0.0)

    first_frame = jnp.where(has_prev, 0, 2)
    col = lax.broadcasted_iota(jnp.int32, (width, channels), 0)

    def activate(slot, row, f):
        v = raw[slot, row, jnp.maximum(f, first_frame)].astype(jnp.float32)
        u = v * coef[row, 0:1, :] + coef[row, 1:2, :]
        y = u * jnp.tanh(u) + u
        left = jnp.where(col == 0, 0.0, pltpu.roll(y, 1, 0))
        right = jnp.where(col == width - 1, 0.0, pltpu.roll(y, width - 1, 0))
        for dj, v in enumerate((left, y, right)):
            act[row, f, :, dj * channels : (dj + 1) * channels] = v.astype(jnp.bfloat16)

    def halo_wait(slot, c, row):
        ok = has_up if row == 0 else has_down
        if c == 0:
            @pl.when(jnp.logical_and(ok, has_prev))
            def _():
                time_copy(slot, 1 if row == 0 else -1).wait_recv()

        @pl.when(ok)
        def _():
            row_copy(slot, c, row == 0).wait_recv()

    def conv_chunk(slot, c):
        new = range(c * CHUNK + 2 if c else 0, c * CHUNK + 5)
        for row in (0, 2):
            halo_wait(slot, c, row)
        for f in new:
            activate(slot, 1, f)
        side = [functools.partial(activate, slot, row, f) for f in new for row in (0, 2)]
        total = None
        for n, row in enumerate((1, 0, 2)):
            for k in range(3):
                lhs = act[row, c * CHUNK + k : c * CHUNK + k + CHUNK].reshape(CHUNK * width, 3 * channels)
                part = jnp.dot(lhs, wbuf[slot, k * 3 + row], preferred_element_type=jnp.float32)
                total = part if total is None else total + part
                if n == 0:
                    for work in side[len(side) * k // 3 : len(side) * (k + 1) // 3]:
                        work()
        return total.reshape(CHUNK, width, channels)

    def finish(layer, other, c, y):
        second = lax.rem(layer, 2) == 1
        for f in range(c * CHUNK, (c + 1) * CHUNK):
            h = (y[f - c * CHUNK] + params[0, layer]).astype(jnp.bfloat16).astype(jnp.float32)
            x = xres[f].astype(jnp.float32)
            out = (h + jnp.where(second, x, 0.0)).astype(jnp.bfloat16)
            raw[other, 1, 2 + f] = out
            o_ref[f] = out
            out = out.astype(jnp.float32)
            xres[f] = jnp.where(second, out, x).astype(jnp.bfloat16)
            ssum[0] += fold(out)
            ssum[1] += fold(out * out)

    for copy in small_copies:
        copy.wait()
    for i in range(3):
        for layer in range(LAYERS):
            params[i, layer] = small[i, layer : layer + 1, :]
    with jax.named_scope("entry_wait"):
        pl.semaphore_wait(barrier, n_hp * n_cp - 1)
    with jax.named_scope("send_sums"):
        send_sums(0)
    start_times(0)
    for c in range(n_chunks):
        start_rows(0, c)

    def layer_body(layer, _):
        slot = lax.rem(layer, 2)
        other = 1 - slot
        more = layer < LAYERS - 1

        @pl.when(more)
        def _():
            start_weights(layer + 1, other)

        with jax.named_scope("statistics"):
            statistics(layer)

        with jax.named_scope("w_wait"):
            @pl.when(has_prev)
            def _():
                time_copy(slot, 0).wait_recv()

            for k, di in slab_order:
                weight_copy(layer, slot, k, di).wait()

        ssum[...] = jnp.zeros_like(ssum)
        for c in range(n_chunks):
            with jax.named_scope(f"chunk{c}"):
                finish(layer, other, c, conv_chunk(slot, c))
            if c < n_chunks - 1:
                @pl.when(more)
                def _():
                    start_rows(other, c)

        with jax.named_scope("send_wait"):
            wait_sends(slot)
        @pl.when(more)
        def _():
            with jax.named_scope("send_sums"):
                send_sums(layer + 1)
            with jax.named_scope("send_rest"):
                start_times(other)

                start_rows(other, n_chunks - 1)

        return 0

    lax.fori_loop(0, LAYERS, layer_body, 0)


def solution(mesh):
    n_hp, n_cp = mesh.shape["hp"], mesh.shape["cp"]

    def local_decode(lat, conv_w, conv_b, gn_gamma, gn_beta):
        frames, rows, width, channels = lat.shape
        n_chunks = frames // CHUNK
        total_count = float(frames * n_cp * rows * n_hp * width * (channels // GROUPS))
        hbm_spec = pl.BlockSpec(memory_space=pltpu.HBM)
        bf16, f32 = jnp.bfloat16, jnp.float32
        flops = LAYERS * 2 * frames * width * 27 * channels * channels
        out = pl.pallas_call(
            functools.partial(decode_kernel, n_hp, n_cp, total_count),
            out_shape=jax.ShapeDtypeStruct((frames, width, channels), bf16),
            in_specs=[hbm_spec] * 5,
            out_specs=pl.BlockSpec(memory_space=pltpu.VMEM),
            scratch_shapes=[
                pltpu.VMEM((2, 9, 3 * channels, channels), bf16),
                pltpu.VMEM((2, 3, frames + 2, width, channels), bf16),
                pltpu.VMEM((3, frames + 2, width, 3 * channels), bf16),
                pltpu.VMEM((frames, width, channels), bf16),
                pltpu.VMEM((3, LAYERS, channels), f32),
                pltpu.VMEM((3, LAYERS, 1, channels), f32),
                pltpu.VMEM((2, 8, channels), f32),
                pltpu.VMEM((8, 128), f32),
                pltpu.VMEM((3, 8, channels), f32),
                pltpu.VMEM((LAYERS, 1, 128), f32),
                pltpu.VMEM((LAYERS, n_hp * n_cp, 1, 128), f32),
                pltpu.SemaphoreType.DMA((2, 9)),
                pltpu.SemaphoreType.DMA((2,)),
                pltpu.SemaphoreType.DMA((3,)),
                pltpu.SemaphoreType.DMA((2, 3, n_chunks + 1)),
                pltpu.SemaphoreType.DMA((2, 3, n_chunks + 1)),
                pltpu.SemaphoreType.DMA((LAYERS,)),
                pltpu.SemaphoreType.DMA((LAYERS,)),
            ],
            compiler_params=pltpu.CompilerParams(
                collective_id=0, has_side_effects=True, vmem_limit_bytes=46 * 1024 * 1024),
            cost_estimate=pl.CostEstimate(flops=flops, bytes_accessed=conv_w.size * 2, transcendentals=0),
        )(*(pltpu.with_memory_space_constraint(v, pltpu.HBM) for v in (
            lat.reshape(frames, width, channels), conv_w.reshape(LAYERS, 9, 3 * channels, channels),
            conv_b, gn_gamma, gn_beta)))
        return out.reshape(lat.shape)

    video_spec = P(("dp", "cp"), "hp", None, None)
    return jax.shard_map(local_decode, mesh=mesh, in_specs=(video_spec, P(), P(), P(), P()), out_specs=video_spec, check_vma=False)
```
